16 devices in a mesh: dp: 2 (over y, z), tp: 8 (over x, core).
Axes of the slice: x: 4, y: 2, z: 1, core: 2. Of those that a mesh axis runs over, the one named last changes fastest.
The devices are a block of a 4x4x4 slice.
Arguments:
- x: bfloat16 [128, 7168], P('dp'), parts along dimension 0
- k_cache: bfloat16 [128, 4096, 8, 128], P('dp', None, 'tp'), parts along dimension 0
- v_cache: bfloat16 [128, 4096, 8, 128], P('dp', None, 'tp'), parts along dimension 0
- gain_a: bfloat16 [7168], replicated
- wq: bfloat16 [7168, 7168], P(None, 'tp')
- wo: bfloat16 [7168, 7168], P('tp')
- gain_m: bfloat16 [7168], replicated
- w_gate: bfloat16 [7168, 20480], P(None, 'tp')
- w_up: bfloat16 [7168, 20480], P(None, 'tp')
- w_down: bfloat16 [20480, 7168], P('tp')
Outputs:
- output: bfloat16 [128, 7168], P('dp'), parts along dimension 0
There are 2 independent parts. The reference program is written for one: setup_inputs(seed, part) draws one part's arguments, and reference() takes and returns one part's arrays. A program takes and returns all parts, laid end to end along the dimension named above; an argument that names none is the same for every part.
All inputs are finite; a program needn't handle non-finite values.
Results may differ from the reference program's by a relative error of at most 0.017.
Values are sent between devices in bfloat16 or wider.
A program may use at most 1.5 GiB of HBM per device.

```python
import jax
import jax.numpy as jnp
from jax import lax

BATCH = 64
CACHE = 4096
D = 7168
HEADS = 56
KV_HEADS = 8
HEAD = 128
FF = 20480
THETA = 10000


def setup_inputs(seed: int = 0, part: int = 0) -> dict:
    kx, kc, kw, kn, kq, ko, km, kg, ku, kd = jax.random.split(jax.random.key(seed), 10)
    kx, kc, kw = (jax.random.fold_in(k, part) for k in (kx, kc, kw))

    def weights(key, rows, columns):
        return jax.random.normal(key, (rows, columns), jnp.float32) * rows**-0.5

    drawn = {
        "x": jax.random.normal(kx, (BATCH, D), jnp.float32),
        "k_cache": 2 * jax.random.normal(kc, (BATCH, CACHE, KV_HEADS, HEAD), jnp.float32),
        "v_cache": 4 * jax.random.normal(kw, (BATCH, CACHE, KV_HEADS, HEAD), jnp.float32),
        "gain_a": 1 + 0.1 * jax.random.normal(kn, (D,), jnp.float32),
        "wq": 2 * weights(kq, D, HEADS * HEAD),
        "wo": weights(ko, HEADS * HEAD, D),
        "gain_m": 1 + 0.1 * jax.random.normal(km, (D,), jnp.float32),
        "w_gate": weights(kg, D, FF),
        "w_up": weights(ku, D, FF),
        "w_down": 2 * weights(kd, FF, D),
    }
    return {k: v.astype(jnp.bfloat16) for k, v in drawn.items()}


def normed(x, gain):
    wide = x.astype(jnp.float32)
    scale = lax.rsqrt(jnp.mean(wide * wide, -1, keepdims=True) + 1e-6)
    return (wide * scale * gain.astype(jnp.float32)).astype(jnp.bfloat16)


def turned(t, place, theta):
    half = t.shape[-1] // 2
    angle = place.astype(jnp.float32)[:, None] * theta ** (-jnp.arange(half, dtype=jnp.float32) / half)
    cos, sin = jnp.cos(angle)[:, None], jnp.sin(angle)[:, None]
    a, b = t[..., :half].astype(jnp.float32), t[..., half:].astype(jnp.float32)
    return jnp.concatenate([a * cos - b * sin, b * cos + a * sin], -1).astype(jnp.bfloat16)


def matmul(a, w):
    return jnp.dot(a, w, preferred_element_type=jnp.float32).astype(jnp.bfloat16)


def einsum(form, a, b):
    return jnp.einsum(form, a.astype(jnp.float32), b.astype(jnp.float32))


def seen_by(a, wq, k_cache, v_cache, head, theta):
    batch, cache, kv_heads = k_cache.shape[:3]
    place = jnp.full((batch,), cache - 1)
    q = turned(matmul(a, wq).reshape(batch, -1, head), place, theta).reshape(batch, kv_heads, -1, head)
    scores = einsum("bgsd,bugd->bgsu", q, k_cache) * head**-0.5
    weights = jax.nn.softmax(scores, -1).astype(jnp.bfloat16)
    return einsum("bgsu,bugd->bgsd", weights, v_cache).astype(jnp.bfloat16).reshape(batch, -1)


def hidden_of(b, w_gate, w_up):
    gate = jnp.dot(b, w_gate, preferred_element_type=jnp.float32)
    up = jnp.dot(b, w_up, preferred_element_type=jnp.float32)
    return (jax.nn.silu(gate) * up).astype(jnp.bfloat16)


def reference(x, k_cache, v_cache, gain_a, wq, wo, gain_m, w_gate, w_up, w_down):
    seen = seen_by(normed(x, gain_a), wq, k_cache, v_cache, HEAD, THETA)
    h = (x.astype(jnp.float32) + jnp.dot(seen, wo, preferred_element_type=jnp.float32)).astype(jnp.bfloat16)
    hidden = hidden_of(normed(h, gain_m), w_gate, w_up)
    return (h.astype(jnp.float32) + jnp.dot(hidden, w_down, preferred_element_type=jnp.float32)).astype(jnp.bfloat16)
```

```python
import jax
import jax.numpy as jnp
from jax import lax
from jax.experimental import pallas as pl
from jax.experimental.pallas import tpu as pltpu
from jax.sharding import PartitionSpec as P

HEAD = 128
THETA = 10000
CORES = 2
LANES = 128
TILE = 256
PAIRS = 4
GSLOTS = 10
DSLOTS = 3
MESH = pl.DeviceIdType.MESH
F32, BF16 = jnp.float32, jnp.bfloat16


def dot(a, b):
    return jnp.dot(a, b, preferred_element_type=F32)


def layer_kernel(n, x_hbm, k_hbm, v_hbm, gains, trig, wq_hbm, wo_hbm, wg_hbm, wu_hbm, wd_hbm, out, states, act, h, slots, q, seen, score_a, score_b, hidden, own, a_send, a_recv, b_send, b_recv, x_sem, g_sem, o_sem, k_sem, v_sem, d_sem, a_ssem, a_rsem, b_ssem, b_rsem, c_ssem, c_rsem, p_ssem, p_rsem, y_sem):
    rows, d = x_hbm.shape
    batch, cache = k_hbm.shape[:2]
    width = wq_hbm.shape[1]
    heads = width // HEAD
    ff = wg_hbm.shape[1]
    chips = n // CORES
    chunk = n * LANES
    chunks = d // chunk
    half = chunk // CORES
    pairs = batch // 2
    group = slots.shape[1] // width
    wq_tiles = pl.cdiv(width, TILE)
    wo_first = wq_tiles
    wo_tiles = d // TILE
    wo_slots = pl.cdiv(wo_tiles, group)
    mlp_first = wo_first + wo_slots
    mlp_tiles = 2 * (ff // TILE)

    me = lax.axis_index("tp")
    chip, core = me // CORES, me % CORES
    partner = chip * CORES + (1 - core)

    def chip_at(step):
        return lax.rem(chip + step + chips, chips)

    def wq_copy(t):
        w = min(TILE, width - t * TILE)
        return pltpu.make_async_copy(wq_hbm.at[:, pl.ds(t * TILE, w)], slots.at[t, :, pl.ds(0, w)], g_sem.at[t])

    def wo_place(t):
        return wo_first + t // group, pl.multiple_of((t % group) * width, LANES)

    def wo_copy(t):
        slot, row = wo_place(t)
        return pltpu.make_async_copy(wo_hbm.at[:, pl.ds(pl.multiple_of(t * TILE, TILE), TILE)], slots.at[slot, pl.ds(row, width)], o_sem.at[t])

    def mlp_slot(t):
        return lax.rem(t + mlp_first, GSLOTS)

    def mlp_copy(w_hbm, t):
        slot = mlp_slot(t)
        return pltpu.make_async_copy(w_hbm.at[:, pl.ds(pl.multiple_of((t // 2) * TILE, TILE), TILE)], slots.at[slot], g_sem.at[slot])

    def mlp_start(j):
        mlp_copy(wg_hbm, 2 * j).start()
        mlp_copy(wu_hbm, 2 * j + 1).start()

    x_copy = pltpu.make_async_copy(x_hbm, states, x_sem)
    x_copy.start()
    for t in range(wq_tiles):
        wq_copy(t).start()

    def normed(src, gain_row):
        squares = jnp.zeros((rows, LANES), F32)
        for c in range(d // LANES):
            wide = src[:, c * LANES : (c + 1) * LANES].astype(F32)
            squares += wide * wide
        scale = lax.rsqrt(jnp.sum(squares, -1, keepdims=True) / d + 1e-6)
        for c in range(d // LANES):
            at = slice(c * LANES, (c + 1) * LANES)
            act[:, at] = (src[:, at].astype(F32) * scale * gains[gain_row : gain_row + 1, at]).astype(BF16)

    def attention(keys, values):
        def k_copy(p):
            slot = lax.rem(p, PAIRS)
            return pltpu.make_async_copy(k_hbm.at[pl.ds(2 * p, 2)], keys.at[slot], k_sem.at[slot])

        def v_copy(p):
            slot = lax.rem(p, PAIRS)
            return pltpu.make_async_copy(v_hbm.at[pl.ds(2 * p, 2)], values.at[slot], v_sem.at[slot])

        for p in range(PAIRS):
            k_copy(p).start()
            v_copy(p).start()

        @pl.loop(0, wo_tiles)
        def _(t):
            wo_copy(t).start()

        barrier = pltpu.get_barrier_semaphore()
        pl.semaphore_signal(barrier, inc=1, device_id={"tp": partner}, device_id_type=MESH)
        for step in range(1, chips):
            pl.semaphore_signal(barrier, inc=1, device_id={"tp": chip_at(step) * CORES + core}, device_id_type=MESH)

        x_copy.wait()
        normed(states, 0)
        for t in range(wq_tiles):
            wq_copy(t).wait()
            w = min(TILE, width - t * TILE)
            qt = dot(act[...], slots[t, :, :w]).astype(BF16).astype(F32)
            for i in range(w // HEAD):
                one = qt[:, i * HEAD : (i + 1) * HEAD]
                turned = one * trig[0:1] + pltpu.roll(one, HEAD // 2, 1) * trig[1:2]
                q[pl.ds(t * (TILE // HEAD) + i, rows, stride=8), :] = turned.astype(BF16).astype(F32)
        for i in range(heads, 8):
            q[pl.ds(i, rows, stride=8), :] = jnp.zeros((rows, HEAD), F32)

        step_keys = 512

        def scores(p, dst):
            slot = lax.rem(p, PAIRS)
            first = q[pl.ds(pl.multiple_of(16 * p, 16), 8), :]
            second = q[pl.ds(pl.multiple_of(16 * p + 8, 8), 8), :]
            zero = jnp.zeros_like(first)
            both = jnp.concatenate([jnp.concatenate([first, zero], 1), jnp.concatenate([zero, second], 1)], 0).astype(BF16)
            for c in range(0, cache, step_keys):
                at = slice(c, c + step_keys)
                k2 = jnp.concatenate([keys[slot, 0, at], keys[slot, 1, at]], 1)
                dst[:, at] = lax.dot_general(both, k2, (((1,), (1,)), ((), ())), preferred_element_type=F32)

        def weighted(p, src):
            slot = lax.rem(p, PAIRS)
            s = src[...]
            e = jnp.exp((s - jnp.max(s, -1, keepdims=True)) * HEAD**-0.5)
            weights = (e * (1 / jnp.sum(e, -1, keepdims=True))).astype(BF16)
            v2 = jnp.concatenate([values[slot, 0], values[slot, 1]], 1)
            o = dot(weights, v2)
            seen[pl.ds(pl.multiple_of(16 * p, 16), 8), :] = o[:8, :HEAD]
            seen[pl.ds(pl.multiple_of(16 * p + 8, 8), 8), :] = o[8:, HEAD:]

        k_copy(0).wait()
        scores(0, score_a)
        k_copy(PAIRS).start()

        trips = pairs // 2
        ahead = (trips - 1) - mlp_first_pairs

        def trip(i, last):
            p = 2 * i
            k_copy(p + 1).wait()
            if not last:
                k_copy(p + 2).wait()
            v_copy(p).wait()
            v_copy(p + 1).wait()
            weighted(p, score_a)
            scores(p + 1, score_b)
            if not last:
                scores(p + 2, score_a)
            weighted(p + 1, score_b)

        @pl.loop(0, trips - 1)
        def _(i):
            trip(i, False)

            @pl.when(2 * i + PAIRS + 1 < pairs)
            def _():
                for s in range(2):
                    v_copy(2 * i + PAIRS + s).start()

            @pl.when(2 * i + PAIRS + 2 < pairs)
            def _():
                k_copy(2 * i + PAIRS + 1).start()
                k_copy(2 * i + PAIRS + 2).start()

            @pl.when(2 * i + PAIRS + 2 == pairs)
            def _():
                k_copy(2 * i + PAIRS + 1).start()

            @pl.when(i >= ahead)
            def _():
                mlp_start(i - ahead)

        trip(trips - 1, True)

    free_first = (GSLOTS - wo_slots) // 2
    mlp_first_pairs = free_first

    def summed(compute, residual, result, lag_b, lag_c, lag_d):
        def columns(c, step):
            return pl.ds(pl.multiple_of(c * chunk + core * half + chip_at(step) * LANES, LANES), LANES)

        def a_copy(c):
            return pltpu.make_async_remote_copy(a_send.at[c], a_recv.at[c], a_ssem.at[c], a_rsem.at[c], device_id={"tp": partner}, device_id_type=MESH)

        def b_copy(c, step):
            to = chip_at(step)
            return pltpu.make_async_remote_copy(b_send.at[c, step - 1], b_recv.at[c, step - 1], b_ssem.at[c, step - 1], b_rsem.at[c, step - 1], device_id={"tp": to * CORES + core}, device_id_type=MESH)

        def c_copy(c, step):
            part = result.at[:, columns(c, 0)]
            return pltpu.make_async_remote_copy(part, part, c_ssem.at[c, step - 1], c_rsem.at[c, step - 1], device_id={"tp": chip_at(step) * CORES + core}, device_id_type=MESH)

        def p_copy(c, step):
            part = result.at[:, columns(c, -step)]
            return pltpu.make_async_remote_copy(part, part, p_ssem.at[c, step], p_rsem.at[c, step], device_id={"tp": partner}, device_id_type=MESH)

        def stage_a(c):
            term = compute(c)
            low, high = term[:, :half], term[:, half:]
            own[c] = jnp.where(core == 0, low, high)
            a_send[c] = jnp.where(core == 0, high, low).astype(BF16)
            a_copy(c).start()

        def stage_b(c):
            a_copy(c).wait_recv()
            own[c] = own[c] + a_recv[c].astype(F32)
            for step in range(1, chips):
                b_send[c, step - 1] = own[c, :, pl.ds(pl.multiple_of(chip_at(step) * LANES, LANES), LANES)].astype(BF16)
                b_copy(c, step).start()

        def stage_c(c):
            total = own[c, :, pl.ds(pl.multiple_of(chip * LANES, LANES), LANES)]
            for step in range(1, chips):
                b_copy(c, step).wait_recv()
                total += b_recv[c, step - 1].astype(F32)
            mine = columns(c, 0)
            result[:, mine] = (residual[:, mine].astype(F32) + total).astype(BF16)
            for step in range(1, chips):
                c_copy(c, step).start()
            p_copy(c, 0).start()

        def stage_d(c):
            for step in range(1, chips):
                c_copy(c, step).wait_recv()
                p_copy(c, step).start()

        @pl.loop(0, chunks + lag_d)
        def _(i):
            for stage, lag in ((stage_a, 0), (stage_b, lag_b), (stage_c, lag_c), (stage_d, lag_d)):
                pl.when((i >= lag) & (i < chunks + lag))(lambda stage=stage, lag=lag: stage(i - lag))

        def finish(c):
            for step in range(chips):
                p_copy(c, step).wait_recv()

        def drain(c):
            a_copy(c).wait_send()
            for step in range(1, chips):
                b_copy(c, step).wait_send()
                c_copy(c, step).wait_send()
            for step in range(chips):
                p_copy(c, step).wait_send()

        return finish, drain

    def rest(down):
        def d_copy(c):
            slot = lax.rem(c, DSLOTS)
            return pltpu.make_async_copy(wd_hbm.at[:, pl.ds(pl.multiple_of(c * chunk, chunk), chunk)], down.at[slot], d_sem.at[slot])

        for c in range(DSLOTS):
            d_copy(c).start()

        pl.semaphore_wait(pltpu.get_barrier_semaphore(), chips)

        for i in range(heads):
            hidden[:, i * HEAD : (i + 1) * HEAD] = seen[pl.ds(i, rows, stride=8), :].astype(BF16)

        def wo_term(c):
            parts = []
            for i in range(chunk // TILE):
                t = c * (chunk // TILE) + i
                wo_copy(t).wait()
                slot, row = wo_place(t)
                parts.append(dot(hidden[:, :width], slots[slot, pl.ds(row, width)]))
            term = jnp.concatenate(parts, 1)

            @pl.when(c == chunks - 1)
            def _():
                @pl.loop(free_first, GSLOTS // 2)
                def _(j):
                    mlp_start(j)

            return term

        finish, drain = summed(wo_term, states, h, 2, chunks, chunks + 4)

        @pl.loop(0, chunks)
        def _(c):
            finish(c)
            drain(c)

        normed(h, 1)

        @pl.loop(0, mlp_tiles // 2)
        def _(j):
            mlp_copy(wg_hbm, 2 * j).wait()
            mlp_copy(wu_hbm, 2 * j + 1).wait()
            gate = dot(act[...], slots[mlp_slot(2 * j)])
            up = dot(act[...], slots[mlp_slot(2 * j + 1)])
            hidden[:, pl.ds(pl.multiple_of(j * TILE, TILE), TILE)] = (gate * (1 / (1 + jnp.exp(-gate))) * up).astype(BF16)

            @pl.when(2 * j + GSLOTS < mlp_tiles)
            def _():
                mlp_start(j + GSLOTS // 2)

        def down_term(c):
            d_copy(c).wait()
            term = dot(hidden[...], down[lax.rem(c, DSLOTS)])

            @pl.when(c + DSLOTS < chunks)
            def _():
                d_copy(c + DSLOTS).start()

            return term

        finish, drain = summed(down_term, h, states, 1, 3, 5)

        def y_copy(c):
            at = pl.ds(pl.multiple_of(c * chunk, chunk), chunk)
            return pltpu.make_async_copy(states.at[:, at], out.at[:, at], y_sem.at[c])

        @pl.loop(0, chunks)
        def _(c):
            finish(c)
            y_copy(c).start()

        @pl.loop(0, chunks)
        def _(c):
            drain(c)
            y_copy(c).wait()

    pl.run_scoped(attention, pltpu.VMEM((PAIRS, 2, cache, HEAD), BF16), pltpu.VMEM((PAIRS, 2, cache, HEAD), BF16))
    pl.run_scoped(rest, pltpu.VMEM((DSLOTS, ff, chunk), BF16))


def solution(mesh):
    n = mesh.shape["tp"]

    def step(x, k_cache, v_cache, gain_a, wq, wo, gain_m, w_gate, w_up, w_down):
        rows, d = x.shape
        batch, cache, kv_heads, head = k_cache.shape
        ff = w_gate.shape[1]
        chips = n // CORES
        chunk = n * LANES
        chunks = d // chunk
        half = head // 2
        angle = jnp.full((1,), cache - 1).astype(F32)[:, None] * THETA ** (-jnp.arange(half, dtype=F32) / half)
        cos, sin = jnp.cos(angle), jnp.sin(angle)
        trig = jnp.concatenate([jnp.concatenate([cos, cos], 1), jnp.concatenate([-sin, sin], 1)], 0)
        gains = jnp.stack([gain_a, gain_m]).astype(F32)
        dma, vmem = pltpu.SemaphoreType.DMA, pltpu.VMEM
        in_hbm = pl.BlockSpec(memory_space=pl.ANY)
        in_vmem = pl.BlockSpec(memory_space=pltpu.VMEM)
        return pl.pallas_call(
            lambda *refs: layer_kernel(n, *refs),
            out_shape=jax.ShapeDtypeStruct((rows, d), x.dtype),
            in_specs=[in_hbm] * 3 + [in_vmem] * 2 + [in_hbm] * 5,
            out_specs=in_hbm,
            scratch_shapes=[
                vmem((rows, d), BF16),
                vmem((rows, d), BF16),
                vmem((rows, d), BF16),
                vmem((GSLOTS, d, TILE), BF16),
                vmem((batch * 8, head), F32),
                vmem((batch * 8, head), F32),
                vmem((16, cache), F32),
                vmem((16, cache), F32),
                vmem((rows, ff), BF16),
                vmem((chunks, rows, chunk // CORES), F32),
                vmem((chunks, rows, chunk // CORES), BF16),
                vmem((chunks, rows, chunk // CORES), BF16),
                vmem((chunks, chips - 1, rows, LANES), BF16),
                vmem((chunks, chips - 1, rows, LANES), BF16),
                dma,
                dma((GSLOTS,)),
                dma((d // TILE,)),
                dma((PAIRS,)),
                dma((PAIRS,)),
                dma((DSLOTS,)),
                dma((chunks,)),
                dma((chunks,)),
                dma((chunks, chips - 1)),
                dma((chunks, chips - 1)),
                dma((chunks, chips - 1)),
                dma((chunks, chips - 1)),
                dma((chunks, chips)),
                dma((chunks, chips)),
                dma((chunks,)),
            ],
            compiler_params=pltpu.CompilerParams(collective_id=0, has_side_effects=True, vmem_limit_bytes=67_043_328),
            name="decoder_layer",
        )(x, k_cache.reshape(batch, cache, head), v_cache.reshape(batch, cache, head), gains, trig, wq, wo, w_gate, w_up, w_down)

    states, cache, columns, rows_of = P("dp", None), P("dp", None, "tp", None), P(None, "tp"), P("tp", None)
    return jax.shard_map(
        step,
        mesh=mesh,
        in_specs=(states, cache, cache, P(None), columns, rows_of, P(None), columns, columns, rows_of),
        out_specs=states,
        check_vma=False,
    )
```

```python
import jax
import jax.numpy as jnp
from jax import lax
from jax.experimental import pallas as pl
from jax.experimental.pallas import tpu as pltpu
from jax.sharding import PartitionSpec as P

HEAD = 128
THETA = 10000
CORES = 2
LANES = 128
TILE = 256
PAIRS = 5
GSLOTS = 10
DSLOTS = 3
H_LAGS = (0, 3, 10, 17)
Y_LAGS = (0, 1, 4, 7)
MESH = pl.DeviceIdType.MESH
F32, BF16 = jnp.float32, jnp.bfloat16
scope = jax.named_scope


def dot(a, b):
    return jnp.dot(a, b, preferred_element_type=F32)


def layer_kernel(n, x_hbm, k_hbm, v_hbm, gain_a_hbm, gain_m_hbm, cos, sin, wq_hbm, wo_hbm, wg_hbm, wu_hbm, wd_hbm, out, states, act, h, gains, slots, q, seen, score_a, score_b, hidden, own, a_send, a_recv, b_send, b_recv, x_sem, gain_sem, g_sem, o_sem, k_sem, v_sem, d_sem, a_rsem, b_rsem, c_rsem, p_rsem, send_sem, y_sem):
    rows, d = x_hbm.shape
    batch, cache = k_hbm.shape[:2]
    width = wq_hbm.shape[1]
    heads = width // HEAD
    ff = wg_hbm.shape[1]
    chips = n // CORES
    chunk = n * LANES
    chunks = d // chunk
    half = chunk // CORES
    pairs = batch // 2
    trips = pairs // 2
    wq_tiles = pl.cdiv(width, TILE)
    tall = width * (chunk // TILE)
    per_slot = slots.shape[1] // tall
    wo_first = wq_tiles
    wo_slots = pl.cdiv(chunks, per_slot)
    mlp_first = wo_first + wo_slots
    mlp_tiles = 2 * (ff // TILE)
    free_first = (GSLOTS - wo_slots) // 2

    me = lax.axis_index("tp")
    chip, core = me // CORES, me % CORES
    partner = chip * CORES + (1 - core)

    def chip_at(step):
        return lax.rem(chip + step + chips, chips)

    def wq_copy(t):
        w = min(TILE, width - t * TILE)
        return pltpu.make_async_copy(wq_hbm.at[:, pl.ds(t * TILE, w)], slots.at[t, :, pl.ds(0, w)], g_sem.at[t])

    def wo_place(c):
        return wo_first + c // per_slot, (c % per_slot) * tall

    def wo_start(c):
        slot, row = wo_place(c)
        for i in range(chunk // TILE):
            at = pl.ds(pl.multiple_of(row + i * width, LANES), width)
            pltpu.make_async_copy(wo_hbm.at[:, pl.ds(pl.multiple_of(c * chunk + i * TILE, TILE), TILE)], slots.at[slot, at], o_sem.at[c]).start()

    def wo_wait(c):
        slot, row = wo_place(c)
        block = slots.at[slot, pl.ds(pl.multiple_of(row, LANES), tall)]
        pltpu.make_async_copy(block, block, o_sem.at[c]).wait()

    def mlp_slot(t):
        return lax.rem(t + mlp_first, GSLOTS)

    def mlp_copy(w_hbm, t):
        slot = mlp_slot(t)
        return pltpu.make_async_copy(w_hbm.at[:, pl.ds(pl.multiple_of((t // 2) * TILE, TILE), TILE)], slots.at[slot], g_sem.at[slot])

    def mlp_start(j):
        mlp_copy(wg_hbm, 2 * j).start()
        mlp_copy(wu_hbm, 2 * j + 1).start()

    x_copy = pltpu.make_async_copy(x_hbm, states, x_sem)
    x_copy.start()
    gain_copies = [pltpu.make_async_copy(g, gains.at[i], gain_sem.at[i]) for i, g in enumerate((gain_a_hbm, gain_m_hbm))]
    for copy in gain_copies:
        copy.start()
    for t in range(wq_tiles):
        wq_copy(t).start()

    def normed(src, which):
        squares = jnp.zeros((rows, LANES), F32)
        for c in range(d // LANES):
            wide = src[:, c * LANES : (c + 1) * LANES].astype(F32)
            squares += wide * wide
        scale = lax.rsqrt(jnp.sum(squares, -1, keepdims=True) / d + 1e-6)
        gain = gains[which].astype(F32)
        for c in range(d // LANES):
            at = slice(c * LANES, (c + 1) * LANES)
            act[:, at] = (src[:, at].astype(F32) * scale * gain[c : c + 1]).astype(BF16)

    class Summed:
        def __init__(self, name, index, first, count, compute, residual, result):
            self.name, self.index, self.rows, self.compute = name, index, pl.ds(first, count), compute
            self.residual, self.result = residual, result

        def columns(self, c, step):
            return pl.ds(pl.multiple_of(c * chunk + core * half + chip_at(step) * LANES, LANES), LANES)

        def remote(self, src, dst, stage, sem, to):
            return pltpu.make_async_remote_copy(src, dst, send_sem.at[self.index, stage], sem, device_id={"tp": to}, device_id_type=MESH)

        def arrived(self, ref, sem):
            self.remote(ref, ref, 0, sem, partner).wait_recv()

        def stage_a(self, c):
            with scope(self.name + "_term"):
                term = self.compute(c)
            low, high = term[:, :half], term[:, half:]
            own[c, self.rows] = jnp.where(core == 0, low, high)
            a_send[c, self.rows] = jnp.where(core == 0, high, low).astype(BF16)
            self.remote(a_send.at[c, self.rows], a_recv.at[c, self.rows], 0, a_rsem.at[self.index, c], partner).start()

        def stage_b(self, c):
            with scope(self.name + "_a_wait"):
                self.arrived(a_recv.at[c, self.rows], a_rsem.at[self.index, c])
            own[c, self.rows] = own[c, self.rows] + a_recv[c, self.rows].astype(F32)
            for step in range(1, chips):
                b_send[c, step - 1, self.rows] = own[c, self.rows, pl.ds(pl.multiple_of(chip_at(step) * LANES, LANES), LANES)].astype(BF16)
                self.remote(b_send.at[c, step - 1, self.rows], b_recv.at[c, step - 1, self.rows], 1, b_rsem.at[self.index, c], chip_at(step) * CORES + core).start()

        def stage_c(self, c):
            total = own[c, self.rows, pl.ds(pl.multiple_of(chip * LANES, LANES), LANES)]
            with scope(self.name + "_b_wait"):
                self.arrived(b_recv.at[c, :, self.rows], b_rsem.at[self.index, c])
            for step in range(1, chips):
                total += b_recv[c, step - 1, self.rows].astype(F32)
            mine = self.columns(c, 0)
            self.result[self.rows, mine] = (self.residual[self.rows, mine].astype(F32) + total).astype(BF16)
            part = self.result.at[self.rows, mine]
            for step in range(1, chips):
                self.remote(part, part, 2, c_rsem.at[self.index, c], chip_at(step) * CORES + core).start()
            self.remote(part, part, 3, p_rsem.at[self.index, c], partner).start()

        def stage_d(self, c):
            with scope(self.name + "_c_wait"):
                self.arrived(b_recv.at[c, :, self.rows], c_rsem.at[self.index, c])
            for step in range(1, chips):
                part = self.result.at[self.rows, self.columns(c, -step)]
                self.remote(part, part, 3, p_rsem.at[self.index, c], partner).start()

        def stages(self, i, lags):
            for stage, lag in zip((self.stage_a, self.stage_b, self.stage_c, self.stage_d), lags):
                pl.when((i >= lag) & (i < chunks + lag))(lambda stage=stage, lag=lag: stage(i - lag))

        def finish(self, c):
            with scope(self.name + "_p_wait"):
                other = pl.ds(pl.multiple_of(c * chunk + (1 - core) * half, LANES), half)
                self.arrived(self.result.at[self.rows, other], p_rsem.at[self.index, c])

        def drain(self):
            for stage, sent in enumerate((a_send.at[:, self.rows], b_send.at[:, :, self.rows], b_send.at[:, :, self.rows], a_send.at[:, self.rows])):
                self.remote(sent, sent, stage, x_sem, partner).wait_send()

    def gather_heads(first, count):
        for i in range(heads):
            hidden[first : first + count, i * HEAD : (i + 1) * HEAD] = seen[pl.ds(first * 8 + i, count, stride=8), :].astype(BF16)

    def wo_term(first, count):
        def term(c):
            slot, row = wo_place(c)
            a = hidden[first : first + count, :width]
            return jnp.concatenate([dot(a, slots[slot, pl.ds(pl.multiple_of(row + i * width, LANES), width)]) for i in range(chunk // TILE)], 1)

        return term

    early, late = rows // 2, rows - rows // 2
    sums = [Summed("h0", 0, 0, early, wo_term(0, early), states, h), Summed("h1", 1, early, late, wo_term(early, late), states, h)]
    early_trip = trips // 2 - 1
    early_lags = tuple(early_trip + lag for lag in (0, 1, 3, 5))

    def attention(keys, values):
        def k_copy(p):
            slot = lax.rem(p, PAIRS)
            return pltpu.make_async_copy(k_hbm.at[pl.ds(2 * p, 2)], keys.at[slot], k_sem.at[slot])

        def v_copy(p):
            slot = lax.rem(p, PAIRS)
            return pltpu.make_async_copy(v_hbm.at[pl.ds(2 * p, 2)], values.at[slot], v_sem.at[slot])

        for p in range(PAIRS):
            k_copy(p).start()
            v_copy(p).start()

        @pl.loop(0, chunks)
        def _(c):
            wo_start(c)

        barrier = pltpu.get_barrier_semaphore()
        pl.semaphore_signal(barrier, inc=1, device_id={"tp": partner}, device_id_type=MESH)
        for step in range(1, chips):
            pl.semaphore_signal(barrier, inc=1, device_id={"tp": chip_at(step) * CORES + core}, device_id_type=MESH)

        with scope("x_wait"):
            x_copy.wait()
            for copy in gain_copies:
                copy.wait()
        with scope("norm_a"):
            normed(states, 0)
        for t in range(wq_tiles):
            with scope("wq_wait"):
                wq_copy(t).wait()
            w = min(TILE, width - t * TILE)
            qt = dot(act[...], slots[t, :, :w]).astype(BF16).astype(F32)
            for i in range(w // HEAD):
                one = qt[:, i * HEAD : (i + 1) * HEAD]
                turned = one * jnp.concatenate([cos[...], cos[...]], 1) + pltpu.roll(one, HEAD // 2, 1) * jnp.concatenate([-sin[...], sin[...]], 1)
                q[pl.ds(t * (TILE // HEAD) + i, rows, stride=8), :] = turned.astype(BF16).astype(F32)
        for i in range(heads, 8):
            q[pl.ds(i, rows, stride=8), :] = jnp.zeros((rows, HEAD), F32)

        step_keys = 512

        def scores(p, dst):
            slot = lax.rem(p, PAIRS)
            first = q[pl.ds(pl.multiple_of(16 * p, 16), 8), :]
            second = q[pl.ds(pl.multiple_of(16 * p + 8, 8), 8), :]
            zero = jnp.zeros_like(first)
            both = jnp.concatenate([jnp.concatenate([first, zero], 1), jnp.concatenate([zero, second], 1)], 0).astype(BF16)
            for c in range(0, cache, step_keys):
                at = slice(c, c + step_keys)
                k2 = jnp.concatenate([keys[slot, 0, at], keys[slot, 1, at]], 1)
                dst[:, at] = lax.dot_general(both, k2, (((1,), (1,)), ((), ())), preferred_element_type=F32)

        def weighted(p, src):
            slot = lax.rem(p, PAIRS)
            s = src[...]
            e = jnp.exp((s - jnp.max(s, -1, keepdims=True)) * HEAD**-0.5)
            weights = (e * (1 / jnp.sum(e, -1, keepdims=True))).astype(BF16)
            v2 = jnp.concatenate([values[slot, 0], values[slot, 1]], 1)
            o = dot(weights, v2)
            seen[pl.ds(pl.multiple_of(16 * p, 16), 8), :] = o[:8, :HEAD]
            seen[pl.ds(pl.multiple_of(16 * p + 8, 8), 8), :] = o[8:, HEAD:]

        with scope("k0_wait"):
            k_copy(0).wait()
        with scope("scores0"):
            scores(0, score_a)
        k_copy(PAIRS).start()
        with scope("wo_wait"):
            for c in range(chunks):
                wo_wait(c)
        with scope("barrier"):
            pl.semaphore_wait(pltpu.get_barrier_semaphore(), chips)

        def trip(i, last):
            p = 2 * i
            with scope("trip_wait"):
                k_copy(p + 1).wait()
                if not last:
                    k_copy(p + 2).wait()
                v_copy(p).wait()
                v_copy(p + 1).wait()
            with scope("trip"):
                weighted(p, score_a)
                scores(p + 1, score_b)
                if not last:
                    scores(p + 2, score_a)
                weighted(p + 1, score_b)

        @pl.loop(0, trips - 1)
        def _(i):
            trip(i, False)
            for s in range(2):
                pl.when(2 * i + s + PAIRS < pairs)(lambda s=s: v_copy(2 * i + s + PAIRS).start())
                pl.when(2 * i + s + 1 + PAIRS < pairs)(lambda s=s: k_copy(2 * i + s + 1 + PAIRS).start())

            @pl.when(i >= trips - 1 - free_first)
            def _():
                mlp_start(i - (trips - 1 - free_first))

            pl.when(i == early_trip)(lambda: gather_heads(0, early))
            sums[0].stages(i, early_lags)

        trip(trips - 1, True)
        gather_heads(early, late)

    def rest(down):
        def d_copy(c):
            slot = lax.rem(c, DSLOTS)
            return pltpu.make_async_copy(wd_hbm.at[:, pl.ds(pl.multiple_of(c * chunk, chunk), chunk)], down.at[slot], d_sem.at[slot])

        for c in range(DSLOTS):
            d_copy(c).start()

        @pl.loop(0, chunks + H_LAGS[-1])
        def _(i):
            sums[1].stages(i, H_LAGS)

            @pl.when(i == chunks - 1)
            def _():
                @pl.loop(free_first, GSLOTS // 2)
                def _(j):
                    mlp_start(j)

            sums[0].stages(i + trips - 1, early_lags)

        for one in sums:
            pl.loop(0, chunks)(one.finish)
            one.drain()

        with scope("norm_m"):
            normed(h, 1)

        @pl.loop(0, mlp_tiles // 2, step=2)
        def _(j):
            with scope("mlp_wait"):
                for s in range(2):
                    mlp_copy(wg_hbm, 2 * (j + s)).wait()
                    mlp_copy(wu_hbm, 2 * (j + s) + 1).wait()
            with scope("mlp"):
                for s in range(2):
                    gate = dot(act[...], slots[mlp_slot(2 * (j + s))])
                    up = dot(act[...], slots[mlp_slot(2 * (j + s) + 1)])
                    hidden[:, pl.ds(pl.multiple_of((j + s) * TILE, TILE), TILE)] = (gate * (1 / (1 + jnp.exp(-gate))) * up).astype(BF16)

            for s in range(2):
                pl.when(2 * (j + s) + GSLOTS < mlp_tiles)(lambda s=s: mlp_start(j + s + GSLOTS // 2))

        def down_term(c):
            with scope("down_wait"):
                d_copy(c).wait()
            term = dot(hidden[...], down[lax.rem(c, DSLOTS)])

            @pl.when(c + DSLOTS < chunks)
            def _():
                d_copy(c + DSLOTS).start()

            return term

        y = Summed("y", 0, 0, rows, down_term, h, states)

        @pl.loop(0, chunks + Y_LAGS[-1])
        def _(i):
            y.stages(i, Y_LAGS)

        @pl.loop(0, chunks)
        def _(c):
            y.finish(c)
            at = pl.ds(pl.multiple_of(c * chunk, chunk), chunk)
            pltpu.make_async_copy(states.at[:, at], out.at[:, at], y_sem).start()

        with scope("y_out"):
            y.drain()
            pltpu.make_async_copy(states, out, y_sem).wait()

    pl.run_scoped(attention, pltpu.VMEM((PAIRS, 2, cache, HEAD), BF16), pltpu.VMEM((PAIRS, 2, cache, HEAD), BF16))
    pl.run_scoped(rest, pltpu.VMEM((DSLOTS, ff, chunk), BF16))


def solution(mesh):
    n = mesh.shape["tp"]

    def step(x, k_cache, v_cache, gain_a, wq, wo, gain_m, w_gate, w_up, w_down):
        rows, d = x.shape
        batch, cache, kv_heads, head = k_cache.shape
        ff = w_gate.shape[1]
        chips = n // CORES
        chunk = n * LANES
        chunks = d // chunk
        half = head // 2
        angle = jnp.full((1,), cache - 1).astype(F32)[:, None] * THETA ** (-jnp.arange(half, dtype=F32) / half)
        cos, sin = jnp.cos(angle), jnp.sin(angle)
        dma, vmem = pltpu.SemaphoreType.DMA, pltpu.VMEM
        in_hbm = pl.BlockSpec(memory_space=pl.ANY)
        in_vmem = pl.BlockSpec(memory_space=pltpu.VMEM)
        return pl.pallas_call(
            lambda *refs: layer_kernel(n, *refs),
            out_shape=jax.ShapeDtypeStruct((rows, d), x.dtype),
            in_specs=[in_hbm] * 5 + [in_vmem] * 2 + [in_hbm] * 5,
            out_specs=in_hbm,
            scratch_shapes=[
                vmem((rows, d), BF16),
                vmem((rows, d), BF16),
                vmem((rows, d), BF16),
                vmem((2, d // LANES, LANES), BF16),
                vmem((GSLOTS, d, TILE), BF16),
                vmem((batch * 8, head), F32),
                vmem((batch * 8, head), F32),
                vmem((16, cache), F32),
                vmem((16, cache), F32),
                vmem((rows, ff), BF16),
                vmem((chunks, rows, chunk // CORES), F32),
                vmem((chunks, rows, chunk // CORES), BF16),
                vmem((chunks, rows, chunk // CORES), BF16),
                vmem((chunks, chips - 1, rows, LANES), BF16),
                vmem((chunks, chips - 1, rows, LANES), BF16),
                dma,
                dma((2,)),
                dma((GSLOTS,)),
                dma((chunks,)),
                dma((PAIRS,)),
                dma((PAIRS,)),
                dma((DSLOTS,)),
                dma((2, chunks)),
                dma((2, chunks)),
                dma((2, chunks)),
                dma((2, chunks)),
                dma((2, 4)),
                dma,
            ],
            compiler_params=pltpu.CompilerParams(collective_id=0, has_side_effects=True, vmem_limit_bytes=67_043_328),
            name="decoder_layer",
        )(x, k_cache.reshape(batch, cache, head), v_cache.reshape(batch, cache, head), gain_a.reshape(-1, LANES), gain_m.reshape(-1, LANES), cos, sin, wq, wo, w_gate, w_up, w_down)

    states, cache, columns, rows_of = P("dp", None), P("dp", None, "tp", None), P(None, "tp"), P("tp", None)
    return jax.shard_map(
        step,
        mesh=mesh,
        in_specs=(states, cache, cache, P(None), columns, rows_of, P(None), columns, columns, rows_of),
        out_specs=states,
        check_vma=False,
    )
```

```python
import jax
import jax.numpy as jnp
from jax import lax
from jax.experimental import pallas as pl
from jax.experimental.pallas import tpu as pltpu
from jax.sharding import PartitionSpec as P

HEAD = 128
THETA = 10000
CORES = 2
LANES = 128
TILE = 256
PAIRS = 5
GSLOTS = 10
DSLOTS = 4
REST_AT = (0, 0, 5, 9)
H_LAGS = (0, 3, 10, 17)
Y_LAGS = (0, 1, 4, 7)
MESH = pl.DeviceIdType.MESH
F32, BF16 = jnp.float32, jnp.bfloat16
scope = jax.named_scope


def dot(a, b):
    return jnp.dot(a, b, preferred_element_type=F32)


def layer_kernel(n, x_hbm, k_hbm, v_hbm, gain_a_hbm, gain_m_hbm, cos_hbm, sin_hbm, wq_hbm, wo_hbm, wg_hbm, wu_hbm, wd_hbm, states, act, h, slots, q, score_a, score_b, hidden, own, a_send, a_recv, b_send, b_recv, gains, rope, x_sem, gain_sem, g_sem, o_sem, k_sem, v_sem, d_sem, a_rsem, b_rsem, c_rsem, p_rsem, send_sem):
    rows, d = x_hbm.shape
    batch, cache = k_hbm.shape[:2]
    width = wq_hbm.shape[1]
    heads = width // HEAD
    ff = wg_hbm.shape[1]
    chips = n // CORES
    chunk = n * LANES
    chunks = d // chunk
    half = chunk // CORES
    pairs = batch // 2
    trips = pairs // 2
    wq_tiles = pl.cdiv(width, TILE)
    tall = width * (chunk // TILE)
    per_slot = slots.shape[1] // tall
    wo_first = wq_tiles
    wo_slots = pl.cdiv(chunks, per_slot)
    mlp_first = wo_first + wo_slots
    mlp_tiles = 2 * (ff // TILE)
    free_first = (GSLOTS - wo_slots) // 2

    me = lax.axis_index("tp")
    chip, core = me // CORES, me % CORES
    partner = chip * CORES + (1 - core)

    def chip_at(step):
        return lax.rem(chip + step + chips, chips)

    def wq_copy(t):
        w = min(TILE, width - t * TILE)
        return pltpu.make_async_copy(wq_hbm.at[:, pl.ds(t * TILE, w)], slots.at[t, :, pl.ds(0, w)], g_sem.at[t])

    def wo_place(c):
        return wo_first + c // per_slot, (c % per_slot) * tall

    def wo_start(c):
        slot, row = wo_place(c)
        for i in range(chunk // TILE):
            at = pl.ds(pl.multiple_of(row + i * width, LANES), width)
            pltpu.make_async_copy(wo_hbm.at[:, pl.ds(pl.multiple_of(c * chunk + i * TILE, TILE), TILE)], slots.at[slot, at], o_sem.at[c]).start()

    def wo_wait(c):
        slot, row = wo_place(c)
        block = slots.at[slot, pl.ds(pl.multiple_of(row, LANES), tall)]
        pltpu.make_async_copy(block, block, o_sem.at[c]).wait()

    def mlp_slot(t):
        return lax.rem(t + mlp_first, GSLOTS)

    def mlp_copy(w_hbm, t):
        slot = mlp_slot(t)
        return pltpu.make_async_copy(w_hbm.at[:, pl.ds(pl.multiple_of((t // 2) * TILE, TILE), TILE)], slots.at[slot], g_sem.at[slot])

    def mlp_start(j):
        mlp_copy(wg_hbm, 2 * j).start()
        mlp_copy(wu_hbm, 2 * j + 1).start()

    x_copy = pltpu.make_async_copy(x_hbm, states, x_sem)
    x_copy.start()
    small = [(gain_a_hbm, gains.at[0]), (gain_m_hbm, gains.at[1]), (cos_hbm, rope.at[0]), (sin_hbm, rope.at[1])]
    small_copies = [pltpu.make_async_copy(src, dst, gain_sem.at[i]) for i, (src, dst) in enumerate(small)]
    for copy in small_copies:
        copy.start()
    for t in range(2):
        wq_copy(t).start()
    with scope("x_wait"):
        x_copy.wait()
        for copy in small_copies:
            copy.wait()
    for t in range(2, wq_tiles):
        wq_copy(t).start()

    def normed(src, which):
        squares = jnp.zeros((rows, LANES), F32)
        for c in range(d // LANES):
            wide = src[:, c * LANES : (c + 1) * LANES].astype(F32)
            squares += wide * wide
        scale = lax.rsqrt(jnp.sum(squares, -1, keepdims=True) / d + 1e-6)
        gain = gains[which].astype(F32)
        for c in range(d // LANES):
            at = slice(c * LANES, (c + 1) * LANES)
            act[:, at] = (src[:, at].astype(F32) * scale * gain[c : c + 1]).astype(BF16)

    class Summed:
        def __init__(self, name, index, first, count, compute, residual, result):
            self.name, self.index, self.rows, self.compute = name, index, pl.ds(first, count), compute
            self.residual, self.result = residual, result

        def columns(self, c, step):
            return pl.ds(pl.multiple_of(c * chunk + core * half + chip_at(step) * LANES, LANES), LANES)

        def remote(self, src, dst, stage, sem, to):
            return pltpu.make_async_remote_copy(src, dst, send_sem.at[self.index, stage], sem, device_id={"tp": to}, device_id_type=MESH)

        def arrived(self, ref, sem):
            self.remote(ref, ref, 0, sem, partner).wait_recv()

        def stage_a(self, c):
            with scope(self.name + "_term"):
                term = self.compute(c)
            low, high = term[:, :half], term[:, half:]
            own[c, self.rows] = jnp.where(core == 0, low, high)
            a_send[c, self.rows] = jnp.where(core == 0, high, low).astype(BF16)
            self.remote(a_send.at[c, self.rows], a_recv.at[c, self.rows], 0, a_rsem.at[self.index, c], partner).start()

        def stage_b(self, c):
            with scope(self.name + "_a_wait"):
                self.arrived(a_recv.at[c, self.rows], a_rsem.at[self.index, c])
            own[c, self.rows] = own[c, self.rows] + a_recv[c, self.rows].astype(F32)
            for step in range(1, chips):
                b_send[c, step - 1, self.rows] = own[c, self.rows, pl.ds(pl.multiple_of(chip_at(step) * LANES, LANES), LANES)].astype(BF16)
                self.remote(b_send.at[c, step - 1, self.rows], b_recv.at[c, step - 1, self.rows], 1, b_rsem.at[self.index, c], chip_at(step) * CORES + core).start()

        def stage_c(self, c):
            total = own[c, self.rows, pl.ds(pl.multiple_of(chip * LANES, LANES), LANES)]
            with scope(self.name + "_b_wait"):
                self.arrived(b_recv.at[c, :, self.rows], b_rsem.at[self.index, c])
            for step in range(1, chips):
                total += b_recv[c, step - 1, self.rows].astype(F32)
            mine = self.columns(c, 0)
            self.result[self.rows, mine] = (self.residual[self.rows, mine].astype(F32) + total).astype(BF16)
            part = self.result.at[self.rows, mine]
            for step in range(1, chips):
                self.remote(part, part, 2, c_rsem.at[self.index, c], chip_at(step) * CORES + core).start()
            self.remote(part, part, 3, p_rsem.at[self.index, c], partner).start()

        def stage_d(self, c):
            with scope(self.name + "_c_wait"):
                self.arrived(b_recv.at[c, :, self.rows], c_rsem.at[self.index, c])
            for step in range(1, chips):
                part = self.result.at[self.rows, self.columns(c, -step)]
                self.remote(part, part, 3, p_rsem.at[self.index, c], partner).start()

        def stages(self, i, lags, first=(0, 0, 0, 0), last=(chunks,) * 4):
            for stage, lag, lo, hi in zip((self.stage_a, self.stage_b, self.stage_c, self.stage_d), lags, first, last):
                pl.when((i >= lag + lo) & (i < lag + hi))(lambda stage=stage, lag=lag: stage(i - lag))

        def finish(self, c):
            with scope(self.name + "_p_wait"):
                other = pl.ds(pl.multiple_of(c * chunk + (1 - core) * half, LANES), half)
                self.arrived(self.result.at[self.rows, other], p_rsem.at[self.index, c])

        def drain(self):
            for stage, sent in enumerate((a_send.at[:, self.rows], b_send.at[:, :, self.rows], b_send.at[:, :, self.rows], a_send.at[:, self.rows])):
                self.remote(sent, sent, stage, x_sem, partner).wait_send()

    def gather_heads(first, count):
        for i in range(heads):
            hidden[first : first + count, i * HEAD : (i + 1) * HEAD] = q[pl.ds(first * 8 + i, count, stride=8), :].astype(BF16)

    def wo_term(first, count):
        def term(c):
            if first == 0:
                wo_wait(c)
            slot, row = wo_place(c)
            a = hidden[first : first + count, :width]
            return jnp.concatenate([dot(a, slots[slot, pl.ds(pl.multiple_of(row + i * width, LANES), width)]) for i in range(chunk // TILE)], 1)

        return term

    early, late = rows // 2, rows - rows // 2
    sums = [Summed("h0", 0, 0, early, wo_term(0, early), states, h), Summed("h1", 1, early, late, wo_term(early, late), states, h)]
    early_trip = trips // 2 - 1
    early_lags = tuple(early_trip + lag for lag in (0, 1, 3, 5))
    early_done = tuple(min(max(trips - 1 - lag, 0), chunks) for lag in early_lags)
    rest_lags = tuple(at - done for at, done in zip(REST_AT, early_done))

    def attention(keys, values):
        def k_copy(p):
            slot = lax.rem(p, PAIRS)
            return pltpu.make_async_copy(k_hbm.at[pl.ds(2 * p, 2)], keys.at[slot], k_sem.at[slot])

        def v_copy(p):
            slot = lax.rem(p, PAIRS)
            return pltpu.make_async_copy(v_hbm.at[pl.ds(2 * p, 2)], values.at[slot], v_sem.at[slot])

        for p in range(PAIRS):
            k_copy(p).start()
            v_copy(p).start()

        @pl.loop(0, chunks)
        def _(c):
            wo_start(c)

        barrier = pltpu.get_barrier_semaphore()
        pl.semaphore_signal(barrier, inc=1, device_id={"tp": partner}, device_id_type=MESH)
        for step in range(1, chips):
            pl.semaphore_signal(barrier, inc=1, device_id={"tp": chip_at(step) * CORES + core}, device_id_type=MESH)

        with scope("norm_a"):
            normed(states, 0)
        cos = jnp.concatenate([rope[0], rope[0]], 1)
        sin = jnp.concatenate([-rope[1], rope[1]], 1)
        for pair in range(0, wq_tiles, 2):
            tiles = range(pair, min(pair + 2, wq_tiles))
            with scope("wq_wait"):
                for t in tiles:
                    wq_copy(t).wait()
            with scope("wq"):
                parts = [dot(act[...], slots[t, :, : min(TILE, width - t * TILE)]).astype(BF16).astype(F32) for t in tiles]
                for t, part in zip(tiles, parts):
                    for i in range(part.shape[1] // HEAD):
                        one = part[:, i * HEAD : (i + 1) * HEAD]
                        turned = one * cos + pltpu.roll(one, HEAD // 2, 1) * sin
                        q[pl.ds(t * (TILE // HEAD) + i, rows, stride=8), :] = turned.astype(BF16).astype(F32)
        for i in range(heads, 8):
            q[pl.ds(i, rows, stride=8), :] = jnp.zeros((rows, HEAD), F32)

        step_keys = 512

        def scores(p, dst):
            slot = lax.rem(p, PAIRS)
            first = q[pl.ds(pl.multiple_of(16 * p, 16), 8), :]
            second = q[pl.ds(pl.multiple_of(16 * p + 8, 8), 8), :]
            zero = jnp.zeros_like(first)
            both = jnp.concatenate([jnp.concatenate([first, zero], 1), jnp.concatenate([zero, second], 1)], 0).astype(BF16)
            for c in range(0, cache, step_keys):
                at = slice(c, c + step_keys)
                k2 = jnp.concatenate([keys[slot, 0, at], keys[slot, 1, at]], 1)
                dst[:, at] = lax.dot_general(both, k2, (((1,), (1,)), ((), ())), preferred_element_type=F32)

        def weighted(p, src):
            slot = lax.rem(p, PAIRS)
            s = src[...]
            e = jnp.exp((s - jnp.max(s, -1, keepdims=True)) * HEAD**-0.5)
            weights = (e * (1 / jnp.sum(e, -1, keepdims=True))).astype(BF16)
            v2 = jnp.concatenate([values[slot, 0], values[slot, 1]], 1)
            o = dot(weights, v2)
            q[pl.ds(pl.multiple_of(16 * p, 16), 8), :] = o[:8, :HEAD]
            q[pl.ds(pl.multiple_of(16 * p + 8, 8), 8), :] = o[8:, HEAD:]

        with scope("k0_wait"):
            k_copy(0).wait()
        with scope("scores0"):
            scores(0, score_a)
        k_copy(PAIRS).start()
        with scope("barrier"):
            pl.semaphore_wait(pltpu.get_barrier_semaphore(), chips)

        def trip(i, last):
            p = 2 * i
            with scope("trip_wait"):
                k_copy(p + 1).wait()
                if not last:
                    k_copy(p + 2).wait()
                v_copy(p).wait()
                v_copy(p + 1).wait()
            with scope("trip"):
                weighted(p, score_a)
                scores(p + 1, score_b)
                if not last:
                    scores(p + 2, score_a)
                weighted(p + 1, score_b)

        @pl.loop(0, trips - 1)
        def _(i):
            trip(i, False)
            for s in range(2):
                pl.when(2 * i + s + PAIRS < pairs)(lambda s=s: v_copy(2 * i + s + PAIRS).start())
                pl.when(2 * i + s + 1 + PAIRS < pairs)(lambda s=s: k_copy(2 * i + s + 1 + PAIRS).start())

            @pl.when(i >= trips - 1 - free_first)
            def _():
                mlp_start(i - (trips - 1 - free_first))

            pl.when(i == early_trip)(lambda: gather_heads(0, early))
            sums[0].stages(i, early_lags)

        trip(trips - 1, True)
        gather_heads(early, late)

    def rest(down):
        def d_copy(c):
            slot = lax.rem(c, DSLOTS)
            return pltpu.make_async_copy(wd_hbm.at[:, pl.ds(pl.multiple_of(c * chunk, chunk), chunk)], down.at[slot], d_sem.at[slot])

        for c in range(DSLOTS):
            d_copy(c).start()

        @pl.loop(0, chunks + H_LAGS[-1])
        def _(i):
            sums[1].stages(i, H_LAGS)

            @pl.when(i == chunks - 1)
            def _():
                @pl.loop(free_first, GSLOTS // 2)
                def _(j):
                    mlp_start(j)

            sums[0].stages(i, rest_lags, first=early_done)

        for one in sums:
            pl.loop(0, chunks)(one.finish)
            one.drain()

        with scope("norm_m"):
            normed(h, 1)

        @pl.loop(0, mlp_tiles // 2, step=2)
        def _(j):
            with scope("mlp_wait"):
                for s in range(2):
                    mlp_copy(wg_hbm, 2 * (j + s)).wait()
                    mlp_copy(wu_hbm, 2 * (j + s) + 1).wait()
            with scope("mlp"):
                for s in range(2):
                    gate = dot(act[...], slots[mlp_slot(2 * (j + s))])
                    up = dot(act[...], slots[mlp_slot(2 * (j + s) + 1)])
                    hidden[:, pl.ds(pl.multiple_of((j + s) * TILE, TILE), TILE)] = (gate * (1 / (1 + jnp.exp(-gate))) * up).astype(BF16)

            for s in range(2):
                pl.when(2 * (j + s) + GSLOTS < mlp_tiles)(lambda s=s: mlp_start(j + s + GSLOTS // 2))

        def down_term(c):
            with scope("down_wait"):
                d_copy(c).wait()
            slot = lax.rem(c, DSLOTS)
            term = jnp.concatenate([dot(hidden[...], down[slot, :, at : at + 256]) for at in range(0, chunk, 256)], 1)

            @pl.when(c + DSLOTS < chunks)
            def _():
                d_copy(c + DSLOTS).start()

            return term

        y = Summed("y", 0, 0, rows, down_term, h, states)

        @pl.loop(0, chunks + Y_LAGS[-1])
        def _(i):
            y.stages(i, Y_LAGS)

        @pl.loop(0, chunks)
        def _(c):
            y.finish(c)

        with scope("y_drain"):
            y.drain()

    pl.run_scoped(attention, pltpu.VMEM((PAIRS, 2, cache, HEAD), BF16), pltpu.VMEM((PAIRS, 2, cache, HEAD), BF16))
    pl.run_scoped(rest, pltpu.VMEM((DSLOTS, ff, chunk), BF16))


def solution(mesh):
    n = mesh.shape["tp"]

    def step(x, k_cache, v_cache, gain_a, wq, wo, gain_m, w_gate, w_up, w_down):
        rows, d = x.shape
        batch, cache, kv_heads, head = k_cache.shape
        ff = w_gate.shape[1]
        chips = n // CORES
        chunk = n * LANES
        chunks = d // chunk
        half = head // 2
        angle = jnp.full((1,), cache - 1).astype(F32)[:, None] * THETA ** (-jnp.arange(half, dtype=F32) / half)
        cos, sin = jnp.cos(angle), jnp.sin(angle)
        dma, vmem = pltpu.SemaphoreType.DMA, pltpu.VMEM
        in_hbm = pl.BlockSpec(memory_space=pl.ANY)
        return pl.pallas_call(
            lambda *refs: layer_kernel(n, *refs),
            out_shape=pltpu.VMEM((rows, d), x.dtype),
            in_specs=[in_hbm] * 12,
            out_specs=pl.BlockSpec(memory_space=pltpu.VMEM),
            scratch_shapes=[
                vmem((rows, d), BF16),
                vmem((rows, d), BF16),
                vmem((GSLOTS, d, TILE), BF16),
                vmem((batch * 8, head), F32),
                vmem((16, cache), F32),
                vmem((16, cache), F32),
                vmem((rows, ff), BF16),
                vmem((chunks, rows, chunk // CORES), F32),
                vmem((chunks, rows, chunk // CORES), BF16),
                vmem((chunks, rows, chunk // CORES), BF16),
                vmem((chunks, chips - 1, rows, LANES), BF16),
                vmem((chunks, chips - 1, rows, LANES), BF16),
                vmem((2, d // LANES, LANES), BF16),
                vmem((2, 1, half), F32),
                dma,
                dma((4,)),
                dma((GSLOTS,)),
                dma((chunks,)),
                dma((PAIRS,)),
                dma((PAIRS,)),
                dma((DSLOTS,)),
                dma((2, chunks)),
                dma((2, chunks)),
                dma((2, chunks)),
                dma((2, chunks)),
                dma((2, 4)),
            ],
            compiler_params=pltpu.CompilerParams(collective_id=0, has_side_effects=True, vmem_limit_bytes=65_900_000),
            name="decoder_layer",
        )(x, k_cache.reshape(batch, cache, head), v_cache.reshape(batch, cache, head), gain_a.reshape(-1, LANES), gain_m.reshape(-1, LANES), cos, sin, wq, wo, w_gate, w_up, w_down)

    states, cache, columns, rows_of = P("dp", None), P("dp", None, "tp", None), P(None, "tp"), P("tp", None)
    return jax.shard_map(
        step,
        mesh=mesh,
        in_specs=(states, cache, cache, P(None), columns, rows_of, P(None), columns, columns, rows_of),
        out_specs=states,
        check_vma=False,
    )
```

```python
import jax
import jax.numpy as jnp
from jax import lax
from jax.experimental import pallas as pl
from jax.experimental.pallas import tpu as pltpu
from jax.sharding import PartitionSpec as P

HEAD = 128
THETA = 10000
CORES = 2
LANES = 128
TILE = 256
PAIRS = 5
GSLOTS = 10
DSLOTS = 4
MLP_STEP = 1
REST_AT = (0, 0, 2, 9)
H_LAGS = (0, 2, 9, 16)
Y_LAGS = (0, 1, 4, 7)
MESH = pl.DeviceIdType.MESH
F32, BF16 = jnp.float32, jnp.bfloat16
scope = jax.named_scope


def dot(a, b):
    return jnp.dot(a, b, preferred_element_type=F32)


def layer_kernel(n, x_hbm, k_hbm, v_hbm, gain_a_hbm, gain_m_hbm, cos_hbm, sin_hbm, wq_hbm, wo_hbm, wg_hbm, wu_hbm, wd_hbm, states, act, h, slots, q, score_a, score_b, hidden, own, a_send, a_recv, b_send, b_recv, gains, rope, x_sem, gain_sem, g_sem, o_sem, k_sem, v_sem, d_sem, a_rsem, b_rsem, c_rsem, p_rsem, send_sem):
    rows, d = x_hbm.shape
    batch, cache = k_hbm.shape[:2]
    width = wq_hbm.shape[1]
    heads = width // HEAD
    ff = wg_hbm.shape[1]
    chips = n // CORES
    chunk = n * LANES
    chunks = d // chunk
    half = chunk // CORES
    pairs = batch // 2
    trips = pairs // 2
    wq_tiles = pl.cdiv(width, TILE)
    tall = width * (chunk // TILE)
    per_slot = slots.shape[1] // tall
    wo_first = wq_tiles
    wo_slots = pl.cdiv(chunks, per_slot)
    mlp_first = wo_first + wo_slots
    mlp_tiles = 2 * (ff // TILE)
    free_first = (GSLOTS - wo_slots) // 2

    me = lax.axis_index("tp")
    chip, core = me // CORES, me % CORES
    partner = chip * CORES + (1 - core)

    def chip_at(step):
        return lax.rem(chip + step + chips, chips)

    def wq_copy(t):
        w = min(TILE, width - t * TILE)
        return pltpu.make_async_copy(wq_hbm.at[:, pl.ds(t * TILE, w)], slots.at[t, :, pl.ds(0, w)], g_sem.at[t])

    def wo_place(c):
        return wo_first + c // per_slot, (c % per_slot) * tall

    def wo_start(c):
        slot, row = wo_place(c)
        for i in range(chunk // TILE):
            at = pl.ds(pl.multiple_of(row + i * width, LANES), width)
            pltpu.make_async_copy(wo_hbm.at[:, pl.ds(pl.multiple_of(c * chunk + i * TILE, TILE), TILE)], slots.at[slot, at], o_sem.at[c]).start()

    def wo_wait(c):
        slot, row = wo_place(c)
        block = slots.at[slot, pl.ds(pl.multiple_of(row, LANES), tall)]
        pltpu.make_async_copy(block, block, o_sem.at[c]).wait()

    def mlp_slot(t):
        return lax.rem(t + mlp_first, GSLOTS)

    def mlp_copy(w_hbm, t):
        slot = mlp_slot(t)
        return pltpu.make_async_copy(w_hbm.at[:, pl.ds(pl.multiple_of((t // 2) * TILE, TILE), TILE)], slots.at[slot], g_sem.at[slot])

    def mlp_start(j):
        mlp_copy(wg_hbm, 2 * j).start()
        mlp_copy(wu_hbm, 2 * j + 1).start()

    x_copy = pltpu.make_async_copy(x_hbm, states, x_sem)
    x_copy.start()
    small = [(gain_a_hbm, gains.at[0]), (gain_m_hbm, gains.at[1]), (cos_hbm, rope.at[0]), (sin_hbm, rope.at[1])]
    small_copies = [pltpu.make_async_copy(src, dst, gain_sem.at[i]) for i, (src, dst) in enumerate(small)]
    for copy in small_copies:
        copy.start()
    for t in range(2):
        wq_copy(t).start()
    with scope("x_wait"):
        x_copy.wait()
        for copy in small_copies:
            copy.wait()
    for t in range(2, wq_tiles):
        wq_copy(t).start()

    def normed(src, which):
        squares = jnp.zeros((rows, LANES), F32)
        for c in range(d // LANES):
            wide = src[:, c * LANES : (c + 1) * LANES].astype(F32)
            squares += wide * wide
        scale = lax.rsqrt(jnp.sum(squares, -1, keepdims=True) / d + 1e-6)
        gain = gains[which].astype(F32)
        for c in range(d // LANES):
            at = slice(c * LANES, (c + 1) * LANES)
            act[:, at] = (src[:, at].astype(F32) * scale * gain[c : c + 1]).astype(BF16)

    class Summed:
        def __init__(self, name, index, first, count, compute, residual, result):
            self.name, self.index, self.rows, self.compute = name, index, pl.ds(first, count), compute
            self.residual, self.result = residual, result

        def columns(self, c, step):
            return pl.ds(pl.multiple_of(c * chunk + core * half + chip_at(step) * LANES, LANES), LANES)

        def remote(self, src, dst, stage, sem, to):
            return pltpu.make_async_remote_copy(src, dst, send_sem.at[self.index, stage], sem, device_id={"tp": to}, device_id_type=MESH)

        def arrived(self, ref, sem):
            self.remote(ref, ref, 0, sem, partner).wait_recv()

        def stage_a(self, c):
            with scope(self.name + "_term"):
                term = self.compute(c)
            low, high = term[:, :half], term[:, half:]
            own[c, self.rows] = jnp.where(core == 0, low, high)
            a_send[c, self.rows] = jnp.where(core == 0, high, low).astype(BF16)
            self.remote(a_send.at[c, self.rows], a_recv.at[c, self.rows], 0, a_rsem.at[self.index, c], partner).start()

        def stage_b(self, c):
            with scope(self.name + "_a_wait"):
                self.arrived(a_recv.at[c, self.rows], a_rsem.at[self.index, c])
            own[c, self.rows] = own[c, self.rows] + a_recv[c, self.rows].astype(F32)
            for step in range(1, chips):
                b_send[c, step - 1, self.rows] = own[c, self.rows, pl.ds(pl.multiple_of(chip_at(step) * LANES, LANES), LANES)].astype(BF16)
                self.remote(b_send.at[c, step - 1, self.rows], b_recv.at[c, step - 1, self.rows], 1, b_rsem.at[self.index, c], chip_at(step) * CORES + core).start()

        def stage_c(self, c):
            total = own[c, self.rows, pl.ds(pl.multiple_of(chip * LANES, LANES), LANES)]
            with scope(self.name + "_b_wait"):
                self.arrived(b_recv.at[c, :, self.rows], b_rsem.at[self.index, c])
            for step in range(1, chips):
                total += b_recv[c, step - 1, self.rows].astype(F32)
            mine = self.columns(c, 0)
            self.result[self.rows, mine] = (self.residual[self.rows, mine].astype(F32) + total).astype(BF16)
            part = self.result.at[self.rows, mine]
            for step in range(1, chips):
                self.remote(part, part, 2, c_rsem.at[self.index, c], chip_at(step) * CORES + core).start()
            self.remote(part, part, 3, p_rsem.at[self.index, c], partner).start()

        def stage_d(self, c):
            with scope(self.name + "_c_wait"):
                self.arrived(b_recv.at[c, :, self.rows], c_rsem.at[self.index, c])
            for step in range(1, chips):
                part = self.result.at[self.rows, self.columns(c, -step)]
                self.remote(part, part, 3, p_rsem.at[self.index, c], partner).start()

        def stages(self, i, lags, first=(0, 0, 0, 0), last=(chunks,) * 4):
            for stage, lag, lo, hi in zip((self.stage_a, self.stage_b, self.stage_c, self.stage_d), lags, first, last):
                pl.when((i >= lag + lo) & (i < lag + hi))(lambda stage=stage, lag=lag: stage(i - lag))

        def finish(self, c):
            with scope(self.name + "_p_wait"):
                other = pl.ds(pl.multiple_of(c * chunk + (1 - core) * half, LANES), half)
                self.arrived(self.result.at[self.rows, other], p_rsem.at[self.index, c])

        def drain(self):
            for stage, sent in enumerate((a_send.at[:, self.rows], b_send.at[:, :, self.rows], b_send.at[:, :, self.rows], a_send.at[:, self.rows])):
                self.remote(sent, sent, stage, x_sem, partner).wait_send()

    def gather_heads(first, count):
        for i in range(heads):
            hidden[first : first + count, i * HEAD : (i + 1) * HEAD] = q[pl.ds(first * 8 + i, count, stride=8), :].astype(BF16)

    def wo_term(first, count):
        def term(c):
            if first == 0:
                wo_wait(c)
            slot, row = wo_place(c)
            a = hidden[first : first + count, :width]
            return jnp.concatenate([dot(a, slots[slot, pl.ds(pl.multiple_of(row + i * width, LANES), width)]) for i in range(chunk // TILE)], 1)

        return term

    early, late = rows // 2, rows - rows // 2
    sums = [Summed("h0", 0, 0, early, wo_term(0, early), states, h), Summed("h1", 1, early, late, wo_term(early, late), states, h)]
    early_trip = trips // 2 - 1
    early_lags = tuple(early_trip + lag for lag in (0, 1, 3, 5))
    early_done = tuple(min(max(trips - 1 - lag, 0), chunks) for lag in early_lags)
    rest_lags = tuple(at - done for at, done in zip(REST_AT, early_done))

    def attention(keys, values):
        def k_copy(p):
            slot = lax.rem(p, PAIRS)
            return pltpu.make_async_copy(k_hbm.at[pl.ds(2 * p, 2)], keys.at[slot], k_sem.at[slot])

        def v_copy(p):
            slot = lax.rem(p, PAIRS)
            return pltpu.make_async_copy(v_hbm.at[pl.ds(2 * p, 2)], values.at[slot], v_sem.at[slot])

        for p in range(PAIRS):
            k_copy(p).start()
            v_copy(p).start()

        @pl.loop(0, chunks)
        def _(c):
            wo_start(c)

        barrier = pltpu.get_barrier_semaphore()
        pl.semaphore_signal(barrier, inc=1, device_id={"tp": partner}, device_id_type=MESH)
        for step in range(1, chips):
            pl.semaphore_signal(barrier, inc=1, device_id={"tp": chip_at(step) * CORES + core}, device_id_type=MESH)

        with scope("norm_a"):
            normed(states, 0)
        cos = jnp.concatenate([rope[0], rope[0]], 1)
        sin = jnp.concatenate([-rope[1], rope[1]], 1)
        for pair in range(0, wq_tiles, 2):
            tiles = range(pair, min(pair + 2, wq_tiles))
            with scope("wq_wait"):
                for t in tiles:
                    wq_copy(t).wait()
            with scope("wq"):
                parts = [dot(act[...], slots[t, :, : min(TILE, width - t * TILE)]).astype(BF16).astype(F32) for t in tiles]
                for t, part in zip(tiles, parts):
                    for i in range(part.shape[1] // HEAD):
                        one = part[:, i * HEAD : (i + 1) * HEAD]
                        turned = one * cos + pltpu.roll(one, HEAD // 2, 1) * sin
                        q[pl.ds(t * (TILE // HEAD) + i, rows, stride=8), :] = turned.astype(BF16).astype(F32)
        for i in range(heads, 8):
            q[pl.ds(i, rows, stride=8), :] = jnp.zeros((rows, HEAD), F32)

        step_keys = 512

        def scores(p, dst):
            slot = lax.rem(p, PAIRS)
            first = q[pl.ds(pl.multiple_of(16 * p, 16), 8), :]
            second = q[pl.ds(pl.multiple_of(16 * p + 8, 8), 8), :]
            zero = jnp.zeros_like(first)
            both = jnp.concatenate([jnp.concatenate([first, zero], 1), jnp.concatenate([zero, second], 1)], 0).astype(BF16)
            for c in range(0, cache, step_keys):
                at = slice(c, c + step_keys)
                k2 = jnp.concatenate([keys[slot, 0, at], keys[slot, 1, at]], 1)
                dst[:, at] = lax.dot_general(both, k2, (((1,), (1,)), ((), ())), preferred_element_type=F32)

        def weighted(p, src):
            slot = lax.rem(p, PAIRS)
            s = src[...]
            e = jnp.exp((s - jnp.max(s, -1, keepdims=True)) * HEAD**-0.5)
            weights = (e * (1 / jnp.sum(e, -1, keepdims=True))).astype(BF16)
            v2 = jnp.concatenate([values[slot, 0], values[slot, 1]], 1)
            o = dot(weights, v2)
            q[pl.ds(pl.multiple_of(16 * p, 16), 8), :] = o[:8, :HEAD]
            q[pl.ds(pl.multiple_of(16 * p + 8, 8), 8), :] = o[8:, HEAD:]

        with scope("k0_wait"):
            k_copy(0).wait()
        with scope("scores0"):
            scores(0, score_a)
        k_copy(PAIRS).start()
        with scope("barrier"):
            pl.semaphore_wait(pltpu.get_barrier_semaphore(), chips)

        def trip(i, last):
            p = 2 * i
            with scope("trip_wait"):
                k_copy(p + 1).wait()
                if not last:
                    k_copy(p + 2).wait()
                v_copy(p).wait()
                v_copy(p + 1).wait()
            with scope("trip"):
                weighted(p, score_a)
                scores(p + 1, score_b)
                if not last:
                    scores(p + 2, score_a)
                weighted(p + 1, score_b)

        @pl.loop(0, trips - 1)
        def _(i):
            trip(i, False)
            for s in range(2):
                pl.when(2 * i + s + PAIRS < pairs)(lambda s=s: v_copy(2 * i + s + PAIRS).start())
                pl.when(2 * i + s + 1 + PAIRS < pairs)(lambda s=s: k_copy(2 * i + s + 1 + PAIRS).start())

            @pl.when(i >= trips - 1 - free_first)
            def _():
                mlp_start(i - (trips - 1 - free_first))

            pl.when(i == early_trip)(lambda: gather_heads(0, early))
            sums[0].stages(i, early_lags)

        trip(trips - 1, True)
        gather_heads(early, late)

    def rest(down):
        def d_copy(c):
            slot = lax.rem(c, DSLOTS)
            return pltpu.make_async_copy(wd_hbm.at[:, pl.ds(pl.multiple_of(c * chunk, chunk), chunk)], down.at[slot], d_sem.at[slot])

        for c in range(DSLOTS):
            d_copy(c).start()

        @pl.loop(0, chunks + H_LAGS[-1])
        def _(i):
            sums[1].stages(i, H_LAGS)

            @pl.when(i == chunks - 1)
            def _():
                @pl.loop(free_first, GSLOTS // 2)
                def _(j):
                    mlp_start(j)

            sums[0].stages(i, rest_lags, first=early_done)

        for one in sums:
            pl.loop(0, chunks)(one.finish)
            one.drain()

        with scope("norm_m"):
            normed(h, 1)

        @pl.loop(0, mlp_tiles // 2, step=MLP_STEP)
        def _(j):
            with scope("mlp_wait"):
                for s in range(MLP_STEP):
                    mlp_copy(wg_hbm, 2 * (j + s)).wait()
                    mlp_copy(wu_hbm, 2 * (j + s) + 1).wait()
            with scope("mlp"):
                for s in range(MLP_STEP):
                    gate = dot(act[...], slots[mlp_slot(2 * (j + s))])
                    up = dot(act[...], slots[mlp_slot(2 * (j + s) + 1)])
                    hidden[:, pl.ds(pl.multiple_of((j + s) * TILE, TILE), TILE)] = (gate * (1 / (1 + jnp.exp(-gate))) * up).astype(BF16)

            for s in range(MLP_STEP):
                pl.when(2 * (j + s) + GSLOTS < mlp_tiles)(lambda s=s: mlp_start(j + s + GSLOTS // 2))

        def down_term(c):
            with scope("down_wait"):
                d_copy(c).wait()
            slot = lax.rem(c, DSLOTS)
            term = jnp.concatenate([dot(hidden[...], down[slot, :, at : at + 256]) for at in range(0, chunk, 256)], 1)

            @pl.when(c + DSLOTS < chunks)
            def _():
                d_copy(c + DSLOTS).start()

            return term

        y = Summed("y", 0, 0, rows, down_term, h, states)

        @pl.loop(0, chunks + Y_LAGS[-1])
        def _(i):
            y.stages(i, Y_LAGS)

        @pl.loop(0, chunks)
        def _(c):
            y.finish(c)

        with scope("y_drain"):
            y.drain()

    pl.run_scoped(attention, pltpu.VMEM((PAIRS, 2, cache, HEAD), BF16), pltpu.VMEM((PAIRS, 2, cache, HEAD), BF16))
    pl.run_scoped(rest, pltpu.VMEM((DSLOTS, ff, chunk), BF16))


def solution(mesh):
    n = mesh.shape["tp"]

    def step(x, k_cache, v_cache, gain_a, wq, wo, gain_m, w_gate, w_up, w_down):
        rows, d = x.shape
        batch, cache, kv_heads, head = k_cache.shape
        ff = w_gate.shape[1]
        chips = n // CORES
        chunk = n * LANES
        chunks = d // chunk
        half = head // 2
        angle = jnp.full((1,), cache - 1).astype(F32)[:, None] * THETA ** (-jnp.arange(half, dtype=F32) / half)
        cos, sin = jnp.cos(angle), jnp.sin(angle)
        dma, vmem = pltpu.SemaphoreType.DMA, pltpu.VMEM
        in_hbm = pl.BlockSpec(memory_space=pl.ANY)
        return pl.pallas_call(
            lambda *refs: layer_kernel(n, *refs),
            out_shape=pltpu.VMEM((rows, d), x.dtype),
            in_specs=[in_hbm] * 12,
            out_specs=pl.BlockSpec(memory_space=pltpu.VMEM),
            scratch_shapes=[
                vmem((rows, d), BF16),
                vmem((rows, d), BF16),
                vmem((GSLOTS, d, TILE), BF16),
                vmem((batch * 8, head), F32),
                vmem((16, cache), F32),
                vmem((16, cache), F32),
                vmem((rows, ff), BF16),
                vmem((chunks, rows, chunk // CORES), F32),
                vmem((chunks, rows, chunk // CORES), BF16),
                vmem((chunks, rows, chunk // CORES), BF16),
                vmem((chunks, chips - 1, rows, LANES), BF16),
                vmem((chunks, chips - 1, rows, LANES), BF16),
                vmem((2, d // LANES, LANES), BF16),
                vmem((2, 1, half), F32),
                dma,
                dma((4,)),
                dma((GSLOTS,)),
                dma((chunks,)),
                dma((PAIRS,)),
                dma((PAIRS,)),
                dma((DSLOTS,)),
                dma((2, chunks)),
                dma((2, chunks)),
                dma((2, chunks)),
                dma((2, chunks)),
                dma((2, 4)),
            ],
            compiler_params=pltpu.CompilerParams(collective_id=0, has_side_effects=True, vmem_limit_bytes=65_900_000),
            name="decoder_layer",
        )(x, k_cache.reshape(batch, cache, head), v_cache.reshape(batch, cache, head), gain_a.reshape(-1, LANES), gain_m.reshape(-1, LANES), cos, sin, wq, wo, w_gate, w_up, w_down)

    states, cache, columns, rows_of = P("dp", None), P("dp", None, "tp", None), P(None, "tp"), P("tp", None)
    return jax.shard_map(
        step,
        mesh=mesh,
        in_specs=(states, cache, cache, P(None), columns, rows_of, P(None), columns, columns, rows_of),
        out_specs=states,
        check_vma=False,
    )
```

```python
import jax
import jax.numpy as jnp
from jax import lax
from jax.experimental import pallas as pl
from jax.experimental.pallas import tpu as pltpu
from jax.sharding import PartitionSpec as P

HEAD = 128
THETA = 10000
CORES = 2
LANES = 128
TILE = 256
PAIRS = 5
GSLOTS = 10
DSLOTS = 4
WO_AHEAD = 4
MLP_STEP = 1
REST_AT = (0, 0, 2, 9)
H_LAGS = (0, 2, 9, 16)
Y_LAGS = (0, 1, 4, 7)
MESH = pl.DeviceIdType.MESH
F32, BF16 = jnp.float32, jnp.bfloat16
scope = jax.named_scope


def dot(a, b):
    return jnp.dot(a, b, preferred_element_type=F32)


def layer_kernel(n, x_hbm, k_hbm, v_hbm, gain_a_hbm, gain_m_hbm, cos_hbm, sin_hbm, wq_hbm, wo_hbm, wg_hbm, wu_hbm, wd_hbm, states, act, h, slots, q, score_a, score_b, hidden, own, a_send, a_recv, b_send, b_recv, gains, rope, x_sem, gain_sem, g_sem, o_sem, k_sem, v_sem, d_sem, a_rsem, b_rsem, c_rsem, p_rsem, send_sem):
    rows, d = x_hbm.shape
    batch, cache = k_hbm.shape[:2]
    width = wq_hbm.shape[1]
    heads = width // HEAD
    ff = wg_hbm.shape[1]
    chips = n // CORES
    chunk = n * LANES
    chunks = d // chunk
    half = chunk // CORES
    pairs = batch // 2
    trips = pairs // 2
    wq_tiles = pl.cdiv(width, TILE)
    tall = width * (chunk // TILE)
    per_slot = slots.shape[1] // tall
    wo_first = wq_tiles
    wo_slots = pl.cdiv(chunks, per_slot)
    mlp_first = wo_first + wo_slots
    mlp_tiles = 2 * (ff // TILE)
    free_first = (GSLOTS - wo_slots) // 2

    me = lax.axis_index("tp")
    chip, core = me // CORES, me % CORES
    partner = chip * CORES + (1 - core)

    def chip_at(step):
        return lax.rem(chip + step + chips, chips)

    def wq_copy(t):
        w = min(TILE, width - t * TILE)
        return pltpu.make_async_copy(wq_hbm.at[:, pl.ds(t * TILE, w)], slots.at[t, :, pl.ds(0, w)], g_sem.at[t])

    def wo_place(c):
        return wo_first + c // per_slot, (c % per_slot) * tall

    def wo_start(c):
        slot, row = wo_place(c)
        for i in range(chunk // TILE):
            at = pl.ds(pl.multiple_of(row + i * width, LANES), width)
            pltpu.make_async_copy(wo_hbm.at[:, pl.ds(pl.multiple_of(c * chunk + i * TILE, TILE), TILE)], slots.at[slot, at], o_sem.at[c]).start()

    def wo_wait(c):
        slot, row = wo_place(c)
        block = slots.at[slot, pl.ds(pl.multiple_of(row, LANES), tall)]
        pltpu.make_async_copy(block, block, o_sem.at[c]).wait()

    def mlp_slot(t):
        return lax.rem(t + mlp_first, GSLOTS)

    def mlp_copy(w_hbm, t):
        slot = mlp_slot(t)
        return pltpu.make_async_copy(w_hbm.at[:, pl.ds(pl.multiple_of((t // 2) * TILE, TILE), TILE)], slots.at[slot], g_sem.at[slot])

    def mlp_start(j):
        mlp_copy(wg_hbm, 2 * j).start()
        mlp_copy(wu_hbm, 2 * j + 1).start()

    x_copy = pltpu.make_async_copy(x_hbm, states, x_sem)
    x_copy.start()
    small = [(gain_a_hbm, gains.at[0]), (gain_m_hbm, gains.at[1]), (cos_hbm, rope.at[0]), (sin_hbm, rope.at[1])]
    small_copies = [pltpu.make_async_copy(src, dst, gain_sem.at[i]) for i, (src, dst) in enumerate(small)]
    for copy in small_copies:
        copy.start()
    for t in range(2):
        wq_copy(t).start()
    with scope("x_wait"):
        x_copy.wait()
        for copy in small_copies:
            copy.wait()
    for t in range(2, wq_tiles):
        wq_copy(t).start()

    def normed(src, which):
        squares = jnp.zeros((rows, LANES), F32)
        for c in range(d // LANES):
            wide = src[:, c * LANES : (c + 1) * LANES].astype(F32)
            squares += wide * wide
        scale = lax.rsqrt(jnp.sum(squares, -1, keepdims=True) / d + 1e-6)
        gain = gains[which].astype(F32)
        for c in range(d // LANES):
            at = slice(c * LANES, (c + 1) * LANES)
            act[:, at] = (src[:, at].astype(F32) * scale * gain[c : c + 1]).astype(BF16)

    class Summed:
        def __init__(self, name, index, first, count, compute, residual, result):
            self.name, self.index, self.rows, self.compute = name, index, pl.ds(first, count), compute
            self.residual, self.result = residual, result

        def columns(self, c, step):
            return pl.ds(pl.multiple_of(c * chunk + core * half + chip_at(step) * LANES, LANES), LANES)

        def remote(self, src, dst, stage, sem, to):
            return pltpu.make_async_remote_copy(src, dst, send_sem.at[self.index, stage], sem, device_id={"tp": to}, device_id_type=MESH)

        def arrived(self, ref, sem):
            self.remote(ref, ref, 0, sem, partner).wait_recv()

        def stage_a(self, c):
            with scope(self.name + "_term"):
                term = self.compute(c)
            low, high = term[:, :half], term[:, half:]
            own[c, self.rows] = jnp.where(core == 0, low, high)
            a_send[c, self.rows] = jnp.where(core == 0, high, low).astype(BF16)
            self.remote(a_send.at[c, self.rows], a_recv.at[c, self.rows], 0, a_rsem.at[self.index, c], partner).start()

        def stage_b(self, c):
            with scope(self.name + "_a_wait"):
                self.arrived(a_recv.at[c, self.rows], a_rsem.at[self.index, c])
            own[c, self.rows] = own[c, self.rows] + a_recv[c, self.rows].astype(F32)
            for step in range(1, chips):
                b_send[c, step - 1, self.rows] = own[c, self.rows, pl.ds(pl.multiple_of(chip_at(step) * LANES, LANES), LANES)].astype(BF16)
                self.remote(b_send.at[c, step - 1, self.rows], b_recv.at[c, step - 1, self.rows], 1, b_rsem.at[self.index, c], chip_at(step) * CORES + core).start()

        def stage_c(self, c):
            total = own[c, self.rows, pl.ds(pl.multiple_of(chip * LANES, LANES), LANES)]
            with scope(self.name + "_b_wait"):
                self.arrived(b_recv.at[c, :, self.rows], b_rsem.at[self.index, c])
            for step in range(1, chips):
                total += b_recv[c, step - 1, self.rows].astype(F32)
            mine = self.columns(c, 0)
            self.result[self.rows, mine] = (self.residual[self.rows, mine].astype(F32) + total).astype(BF16)
            part = self.result.at[self.rows, mine]
            for step in range(1, chips):
                self.remote(part, part, 2, c_rsem.at[self.index, c], chip_at(step) * CORES + core).start()
            self.remote(part, part, 3, p_rsem.at[self.index, c], partner).start()

        def stage_d(self, c):
            with scope(self.name + "_c_wait"):
                self.arrived(b_recv.at[c, :, self.rows], c_rsem.at[self.index, c])
            for step in range(1, chips):
                part = self.result.at[self.rows, self.columns(c, -step)]
                self.remote(part, part, 3, p_rsem.at[self.index, c], partner).start()

        def stages(self, i, lags, first=(0, 0, 0, 0), last=(chunks,) * 4):
            for stage, lag, lo, hi in zip((self.stage_a, self.stage_b, self.stage_c, self.stage_d), lags, first, last):
                pl.when((i >= lag + lo) & (i < lag + hi))(lambda stage=stage, lag=lag: stage(i - lag))

        def finish(self, c):
            with scope(self.name + "_p_wait"):
                other = pl.ds(pl.multiple_of(c * chunk + (1 - core) * half, LANES), half)
                self.arrived(self.result.at[self.rows, other], p_rsem.at[self.index, c])

        def drain(self):
            for stage, sent in enumerate((a_send.at[:, self.rows], b_send.at[:, :, self.rows], b_send.at[:, :, self.rows], a_send.at[:, self.rows])):
                self.remote(sent, sent, stage, x_sem, partner).wait_send()

    def gather_heads(first, count):
        for i in range(heads):
            hidden[first : first + count, i * HEAD : (i + 1) * HEAD] = q[pl.ds(first * 8 + i, count, stride=8), :].astype(BF16)

    def wo_term(first, count):
        def term(c):
            if first == 0:
                wo_wait(c)
            slot, row = wo_place(c)
            a = hidden[first : first + count, :width]
            return jnp.concatenate([dot(a, slots[slot, pl.ds(pl.multiple_of(row + i * width, LANES), width)]) for i in range(chunk // TILE)], 1)

        return term

    early, late = rows // 2, rows - rows // 2
    sums = [Summed("h0", 0, 0, early, wo_term(0, early), states, h), Summed("h1", 1, early, late, wo_term(early, late), states, h)]
    early_trip = trips // 2 - 1
    early_lags = tuple(early_trip + lag for lag in (0, 1, 3, 5))
    early_done = tuple(min(max(trips - 1 - lag, 0), chunks) for lag in early_lags)
    rest_lags = tuple(at - done for at, done in zip(REST_AT, early_done))

    def attention(keys, values):
        def k_copy(p):
            slot = lax.rem(p, PAIRS)
            return pltpu.make_async_copy(k_hbm.at[pl.ds(2 * p, 2)], keys.at[slot], k_sem.at[slot])

        def v_copy(p):
            slot = lax.rem(p, PAIRS)
            return pltpu.make_async_copy(v_hbm.at[pl.ds(2 * p, 2)], values.at[slot], v_sem.at[slot])

        for p in range(PAIRS):
            k_copy(p).start()
            v_copy(p).start()

        barrier = pltpu.get_barrier_semaphore()
        pl.semaphore_signal(barrier, inc=1, device_id={"tp": partner}, device_id_type=MESH)
        for step in range(1, chips):
            pl.semaphore_signal(barrier, inc=1, device_id={"tp": chip_at(step) * CORES + core}, device_id_type=MESH)

        with scope("norm_a"):
            normed(states, 0)
        cos = jnp.concatenate([rope[0], rope[0]], 1)
        sin = jnp.concatenate([-rope[1], rope[1]], 1)
        for pair in range(0, wq_tiles, 2):
            tiles = range(pair, min(pair + 2, wq_tiles))
            with scope("wq_wait"):
                for t in tiles:
                    wq_copy(t).wait()
            with scope("wq"):
                parts = [dot(act[...], slots[t, :, : min(TILE, width - t * TILE)]).astype(BF16).astype(F32) for t in tiles]
                for t, part in zip(tiles, parts):
                    for i in range(part.shape[1] // HEAD):
                        one = part[:, i * HEAD : (i + 1) * HEAD]
                        turned = one * cos + pltpu.roll(one, HEAD // 2, 1) * sin
                        q[pl.ds(t * (TILE // HEAD) + i, rows, stride=8), :] = turned.astype(BF16).astype(F32)
        for i in range(heads, 8):
            q[pl.ds(i, rows, stride=8), :] = jnp.zeros((rows, HEAD), F32)

        step_keys = 512

        def scores(p, dst):
            slot = lax.rem(p, PAIRS)
            first = q[pl.ds(pl.multiple_of(16 * p, 16), 8), :]
            second = q[pl.ds(pl.multiple_of(16 * p + 8, 8), 8), :]
            zero = jnp.zeros_like(first)
            both = jnp.concatenate([jnp.concatenate([first, zero], 1), jnp.concatenate([zero, second], 1)], 0).astype(BF16)
            for c in range(0, cache, step_keys):
                at = slice(c, c + step_keys)
                k2 = jnp.concatenate([keys[slot, 0, at], keys[slot, 1, at]], 1)
                dst[:, at] = lax.dot_general(both, k2, (((1,), (1,)), ((), ())), preferred_element_type=F32)

        def weighted(p, src):
            slot = lax.rem(p, PAIRS)
            s = src[...]
            e = jnp.exp((s - jnp.max(s, -1, keepdims=True)) * HEAD**-0.5)
            weights = (e * (1 / jnp.sum(e, -1, keepdims=True))).astype(BF16)
            v2 = jnp.concatenate([values[slot, 0], values[slot, 1]], 1)
            o = dot(weights, v2)
            q[pl.ds(pl.multiple_of(16 * p, 16), 8), :] = o[:8, :HEAD]
            q[pl.ds(pl.multiple_of(16 * p + 8, 8), 8), :] = o[8:, HEAD:]

        with scope("k0_wait"):
            k_copy(0).wait()
        with scope("scores0"):
            scores(0, score_a)
        k_copy(PAIRS).start()
        with scope("barrier"):
            pl.semaphore_wait(pltpu.get_barrier_semaphore(), chips)

        def trip(i, last):
            p = 2 * i
            with scope("trip_wait"):
                k_copy(p + 1).wait()
                if not last:
                    k_copy(p + 2).wait()
                v_copy(p).wait()
                v_copy(p + 1).wait()
            with scope("trip"):
                weighted(p, score_a)
                scores(p + 1, score_b)
                if not last:
                    scores(p + 2, score_a)
                weighted(p + 1, score_b)

        @pl.loop(0, trips - 1)
        def _(i):
            trip(i, False)
            for s in range(2):
                pl.when(2 * i + s + PAIRS < pairs)(lambda s=s: v_copy(2 * i + s + PAIRS).start())
                pl.when(2 * i + s + 1 + PAIRS < pairs)(lambda s=s: k_copy(2 * i + s + 1 + PAIRS).start())

            pl.when((i >= early_trip - WO_AHEAD) & (i < early_trip - WO_AHEAD + chunks))(lambda: wo_start(i - (early_trip - WO_AHEAD)))
            pl.when(i >= trips - free_first)(lambda: mlp_start(i - (trips - free_first)))

            pl.when(i == early_trip)(lambda: gather_heads(0, early))
            sums[0].stages(i, early_lags)

        mlp_start(free_first - 1)
        trip(trips - 1, True)
        gather_heads(early, late)

    def rest(down):
        def d_copy(c):
            slot = lax.rem(c, DSLOTS)
            return pltpu.make_async_copy(wd_hbm.at[:, pl.ds(pl.multiple_of(c * chunk, chunk), chunk)], down.at[slot], d_sem.at[slot])

        for c in range(DSLOTS):
            d_copy(c).start()

        @pl.loop(0, chunks + H_LAGS[-1])
        def _(i):
            sums[1].stages(i, H_LAGS)

            @pl.when(i == chunks - 1)
            def _():
                @pl.loop(free_first, GSLOTS // 2)
                def _(j):
                    mlp_start(j)

            sums[0].stages(i, rest_lags, first=early_done)

        for one in sums:
            pl.loop(0, chunks)(one.finish)
            one.drain()

        with scope("norm_m"):
            normed(h, 1)

        @pl.loop(0, mlp_tiles // 2, step=MLP_STEP)
        def _(j):
            with scope("mlp_wait"):
                for s in range(MLP_STEP):
                    mlp_copy(wg_hbm, 2 * (j + s)).wait()
                    mlp_copy(wu_hbm, 2 * (j + s) + 1).wait()
            with scope("mlp"):
                for s in range(MLP_STEP):
                    gate = dot(act[...], slots[mlp_slot(2 * (j + s))])
                    up = dot(act[...], slots[mlp_slot(2 * (j + s) + 1)])
                    hidden[:, pl.ds(pl.multiple_of((j + s) * TILE, TILE), TILE)] = (gate * (1 / (1 + jnp.exp(-gate))) * up).astype(BF16)

            for s in range(MLP_STEP):
                pl.when(2 * (j + s) + GSLOTS < mlp_tiles)(lambda s=s: mlp_start(j + s + GSLOTS // 2))

        def down_term(c):
            with scope("down_wait"):
                d_copy(c).wait()
            slot = lax.rem(c, DSLOTS)
            term = jnp.concatenate([dot(hidden[...], down[slot, :, at : at + 256]) for at in range(0, chunk, 256)], 1)

            @pl.when(c + DSLOTS < chunks)
            def _():
                d_copy(c + DSLOTS).start()

            return term

        y = Summed("y", 0, 0, rows, down_term, h, states)

        @pl.loop(0, chunks + Y_LAGS[-1])
        def _(i):
            y.stages(i, Y_LAGS)

        @pl.loop(0, chunks)
        def _(c):
            y.finish(c)

        with scope("y_drain"):
            y.drain()

    pl.run_scoped(attention, pltpu.VMEM((PAIRS, 2, cache, HEAD), BF16), pltpu.VMEM((PAIRS, 2, cache, HEAD), BF16))
    pl.run_scoped(rest, pltpu.VMEM((DSLOTS, ff, chunk), BF16))


def solution(mesh):
    n = mesh.shape["tp"]

    def step(x, k_cache, v_cache, gain_a, wq, wo, gain_m, w_gate, w_up, w_down):
        rows, d = x.shape
        batch, cache, kv_heads, head = k_cache.shape
        ff = w_gate.shape[1]
        chips = n // CORES
        chunk = n * LANES
        chunks = d // chunk
        half = head // 2
        angle = jnp.full((1,), cache - 1).astype(F32)[:, None] * THETA ** (-jnp.arange(half, dtype=F32) / half)
        cos, sin = jnp.cos(angle), jnp.sin(angle)
        dma, vmem = pltpu.SemaphoreType.DMA, pltpu.VMEM
        in_hbm = pl.BlockSpec(memory_space=pl.ANY)
        return pl.pallas_call(
            lambda *refs: layer_kernel(n, *refs),
            out_shape=pltpu.VMEM((rows, d), x.dtype),
            in_specs=[in_hbm] * 12,
            out_specs=pl.BlockSpec(memory_space=pltpu.VMEM),
            scratch_shapes=[
                vmem((rows, d), BF16),
                vmem((rows, d), BF16),
                vmem((GSLOTS, d, TILE), BF16),
                vmem((batch * 8, head), F32),
                vmem((16, cache), F32),
                vmem((16, cache), F32),
                vmem((rows, ff), BF16),
                vmem((chunks, rows, chunk // CORES), F32),
                vmem((chunks, rows, chunk // CORES), BF16),
                vmem((chunks, rows, chunk // CORES), BF16),
                vmem((chunks, chips - 1, rows, LANES), BF16),
                vmem((chunks, chips - 1, rows, LANES), BF16),
                vmem((2, d // LANES, LANES), BF16),
                vmem((2, 1, half), F32),
                dma,
                dma((4,)),
                dma((GSLOTS,)),
                dma((chunks,)),
                dma((PAIRS,)),
                dma((PAIRS,)),
                dma((DSLOTS,)),
                dma((2, chunks)),
                dma((2, chunks)),
                dma((2, chunks)),
                dma((2, chunks)),
                dma((2, 4)),
            ],
            compiler_params=pltpu.CompilerParams(collective_id=0, has_side_effects=True, vmem_limit_bytes=65_900_000),
            name="decoder_layer",
        )(x, k_cache.reshape(batch, cache, head), v_cache.reshape(batch, cache, head), gain_a.reshape(-1, LANES), gain_m.reshape(-1, LANES), cos, sin, wq, wo, w_gate, w_up, w_down)

    states, cache, columns, rows_of = P("dp", None), P("dp", None, "tp", None), P(None, "tp"), P("tp", None)
    return jax.shard_map(
        step,
        mesh=mesh,
        in_specs=(states, cache, cache, P(None), columns, rows_of, P(None), columns, columns, rows_of),
        out_specs=states,
        check_vma=False,
    )
```

```python
import jax
import jax.numpy as jnp
import numpy as np
from jax import lax
from jax.experimental import pallas as pl
from jax.experimental.pallas import tpu as pltpu
from jax.sharding import PartitionSpec as P

HEAD = 128
THETA = 10000
CORES = 2
LANES = 128
TILE = 256
PAIRS = 5
GSLOTS = 10
DSLOTS = 4
WO_AHEAD = 4
MLP_STEP = 1
Y_LAGS = (0, 1, 4, 7)
MESH = pl.DeviceIdType.MESH
F32, BF16 = jnp.float32, jnp.bfloat16
scope = jax.named_scope


def dot(a, b):
    return jnp.dot(a, b, preferred_element_type=F32)


def layer_kernel(n, x_hbm, k_hbm, v_hbm, gain_a_hbm, gain_m_hbm, cos_hbm, sin_hbm, wq_hbm, wo_hbm, wg_hbm, wu_hbm, wd_hbm, states, act, h, slots, q, score_a, score_b, hidden, own, a_send, a_recv, b_send, b_recv, gains, rope, x_sem, gain_sem, g_sem, o_sem, k_sem, v_sem, d_sem, a_rsem, b_rsem, c_rsem, p_rsem, send_sem):
    rows, d = x_hbm.shape
    batch, cache = k_hbm.shape[:2]
    width = wq_hbm.shape[1]
    heads = width // HEAD
    ff = wg_hbm.shape[1]
    chips = n // CORES
    chunk = n * LANES
    chunks = d // chunk
    half = chunk // CORES
    pairs = batch // 2
    trips = pairs // 2
    wq_tiles = pl.cdiv(width, TILE)
    tall = width * (chunk // TILE)
    per_slot = slots.shape[1] // tall
    wo_first = wq_tiles
    wo_slots = pl.cdiv(chunks, per_slot)
    mlp_first = wo_first + wo_slots
    mlp_tiles = 2 * (ff // TILE)
    free_first = (GSLOTS - wo_slots) // 2

    me = lax.axis_index("tp")
    chip, core = me // CORES, me % CORES
    partner = chip * CORES + (1 - core)

    def chip_at(step):
        return lax.rem(chip + step + chips, chips)

    def wq_copy(t):
        w = min(TILE, width - t * TILE)
        return pltpu.make_async_copy(wq_hbm.at[:, pl.ds(t * TILE, w)], slots.at[t, :, pl.ds(0, w)], g_sem.at[t])

    def wo_place(c):
        return wo_first + c // per_slot, (c % per_slot) * tall

    def wo_start(c):
        slot, row = wo_place(c)
        for i in range(chunk // TILE):
            at = pl.ds(pl.multiple_of(row + i * width, LANES), width)
            pltpu.make_async_copy(wo_hbm.at[:, pl.ds(pl.multiple_of(c * chunk + i * TILE, TILE), TILE)], slots.at[slot, at], o_sem.at[c]).start()

    def wo_wait(c):
        slot, row = wo_place(c)
        block = slots.at[slot, pl.ds(pl.multiple_of(row, LANES), tall)]
        pltpu.make_async_copy(block, block, o_sem.at[c]).wait()

    def mlp_slot(t):
        return lax.rem(t + mlp_first, GSLOTS)

    def mlp_copy(w_hbm, t):
        slot = mlp_slot(t)
        return pltpu.make_async_copy(w_hbm.at[:, pl.ds(pl.multiple_of((t // 2) * TILE, TILE), TILE)], slots.at[slot], g_sem.at[slot])

    def mlp_start(j):
        mlp_copy(wg_hbm, 2 * j).start()
        mlp_copy(wu_hbm, 2 * j + 1).start()

    x_copy = pltpu.make_async_copy(x_hbm, states, x_sem)
    x_copy.start()
    small = [(gain_a_hbm, gains.at[0]), (gain_m_hbm, gains.at[1]), (cos_hbm, rope.at[0]), (sin_hbm, rope.at[1])]
    small_copies = [pltpu.make_async_copy(src, dst, gain_sem.at[i]) for i, (src, dst) in enumerate(small)]
    for copy in small_copies:
        copy.start()
    for t in range(2):
        wq_copy(t).start()
    with scope("x_wait"):
        x_copy.wait()
        for copy in small_copies:
            copy.wait()
    for t in range(2, wq_tiles):
        wq_copy(t).start()

    def normed(src, which):
        squares = jnp.zeros((rows, LANES), F32)
        for c in range(d // LANES):
            wide = src[:, c * LANES : (c + 1) * LANES].astype(F32)
            squares += wide * wide
        scale = lax.rsqrt(jnp.sum(squares, -1, keepdims=True) / d + 1e-6)
        gain = gains[which].astype(F32)
        for c in range(d // LANES):
            at = slice(c * LANES, (c + 1) * LANES)
            act[:, at] = (src[:, at].astype(F32) * scale * gain[c : c + 1]).astype(BF16)

    class Summed:
        def __init__(self, name, index, first, count, compute, residual, result):
            self.name, self.index, self.rows, self.compute = name, index, pl.ds(first, count), compute
            self.residual, self.result = residual, result

        def columns(self, c, step):
            return pl.ds(pl.multiple_of(c * chunk + core * half + chip_at(step) * LANES, LANES), LANES)

        def remote(self, src, dst, stage, sem, to):
            return pltpu.make_async_remote_copy(src, dst, send_sem.at[self.index, stage], sem, device_id={"tp": to}, device_id_type=MESH)

        def arrived(self, ref, sem):
            self.remote(ref, ref, 0, sem, partner).wait_recv()

        def stage_a(self, *cs):
            with scope(self.name + "_term"):
                terms = [self.compute(c) for c in cs]
            for c, term in zip(cs, terms):
                low, high = term[:, :half], term[:, half:]
                own[c, self.rows] = jnp.where(core == 0, low, high)
                a_send[c, self.rows] = jnp.where(core == 0, high, low).astype(BF16)
            for c in cs:
                self.remote(a_send.at[c, self.rows], a_recv.at[c, self.rows], 0, a_rsem.at[self.index, c], partner).start()

        def stage_b(self, c):
            with scope(self.name + "_a_wait"):
                self.arrived(a_recv.at[c, self.rows], a_rsem.at[self.index, c])
            own[c, self.rows] = own[c, self.rows] + a_recv[c, self.rows].astype(F32)
            for step in range(1, chips):
                b_send[c, step - 1, self.rows] = own[c, self.rows, pl.ds(pl.multiple_of(chip_at(step) * LANES, LANES), LANES)].astype(BF16)
                self.remote(b_send.at[c, step - 1, self.rows], b_recv.at[c, step - 1, self.rows], 1, b_rsem.at[self.index, c], chip_at(step) * CORES + core).start()

        def stage_c(self, c):
            total = own[c, self.rows, pl.ds(pl.multiple_of(chip * LANES, LANES), LANES)]
            with scope(self.name + "_b_wait"):
                self.arrived(b_recv.at[c, :, self.rows], b_rsem.at[self.index, c])
            for step in range(1, chips):
                total += b_recv[c, step - 1, self.rows].astype(F32)
            mine = self.columns(c, 0)
            self.result[self.rows, mine] = (self.residual[self.rows, mine].astype(F32) + total).astype(BF16)
            part = self.result.at[self.rows, mine]
            for step in range(1, chips):
                self.remote(part, part, 2, c_rsem.at[self.index, c], chip_at(step) * CORES + core).start()
            self.remote(part, part, 3, p_rsem.at[self.index, c], partner).start()

        def stage_d(self, c):
            with scope(self.name + "_c_wait"):
                self.arrived(b_recv.at[c, :, self.rows], c_rsem.at[self.index, c])
            for step in range(1, chips):
                part = self.result.at[self.rows, self.columns(c, -step)]
                self.remote(part, part, 3, p_rsem.at[self.index, c], partner).start()

        def stages(self, i, lags):
            for stage, lag in zip((self.stage_a, self.stage_b, self.stage_c, self.stage_d), lags):
                pl.when((i >= lag) & (i < lag + chunks))(lambda stage=stage, lag=lag: stage(i - lag))

        def finish(self, c):
            with scope(self.name + "_p_wait"):
                other = pl.ds(pl.multiple_of(c * chunk + (1 - core) * half, LANES), half)
                self.arrived(self.result.at[self.rows, other], p_rsem.at[self.index, c])

        def drain(self):
            for stage, sent in enumerate((a_send.at[:, self.rows], b_send.at[:, :, self.rows], b_send.at[:, :, self.rows], a_send.at[:, self.rows])):
                self.remote(sent, sent, stage, x_sem, partner).wait_send()

    def gather_heads(first, count):
        for i in range(heads):
            hidden[first : first + count, i * HEAD : (i + 1) * HEAD] = q[pl.ds(first * 8 + i, count, stride=8), :].astype(BF16)

    def wo_term(first, count):
        def term(c):
            if first == 0:
                wo_wait(c)
            slot, row = wo_place(c)
            a = hidden[first : first + count, :width]
            return jnp.concatenate([dot(a, slots[slot, pl.ds(pl.multiple_of(row + i * width, LANES), width)]) for i in range(chunk // TILE)], 1)

        return term

    early, late = rows // 2, rows - rows // 2
    sums = [Summed("h0", 0, 0, early, wo_term(0, early), states, h), Summed("h1", 1, early, late, wo_term(early, late), states, h)]
    early_trip = trips // 2 - 1
    early_lags = tuple(early_trip + lag for lag in (0, 1, 3, 5))
    early_done = tuple(min(max(trips - 1 - lag, 0), chunks) for lag in early_lags)

    def attention(keys, values):
        def k_copy(p):
            slot = lax.rem(p, PAIRS)
            return pltpu.make_async_copy(k_hbm.at[pl.ds(2 * p, 2)], keys.at[slot], k_sem.at[slot])

        def v_copy(p):
            slot = lax.rem(p, PAIRS)
            return pltpu.make_async_copy(v_hbm.at[pl.ds(2 * p, 2)], values.at[slot], v_sem.at[slot])

        for p in range(PAIRS):
            k_copy(p).start()
            v_copy(p).start()

        barrier = pltpu.get_barrier_semaphore()
        pl.semaphore_signal(barrier, inc=1, device_id={"tp": partner}, device_id_type=MESH)
        for step in range(1, chips):
            pl.semaphore_signal(barrier, inc=1, device_id={"tp": chip_at(step) * CORES + core}, device_id_type=MESH)

        with scope("norm_a"):
            normed(states, 0)
        cos = jnp.concatenate([rope[0], rope[0]], 1)
        sin = jnp.concatenate([-rope[1], rope[1]], 1)
        for pair in range(0, wq_tiles, 2):
            tiles = range(pair, min(pair + 2, wq_tiles))
            with scope("wq_wait"):
                for t in tiles:
                    wq_copy(t).wait()
            with scope("wq"):
                parts = [dot(act[...], slots[t, :, : min(TILE, width - t * TILE)]).astype(BF16).astype(F32) for t in tiles]
                for t, part in zip(tiles, parts):
                    for i in range(part.shape[1] // HEAD):
                        one = part[:, i * HEAD : (i + 1) * HEAD]
                        turned = one * cos + pltpu.roll(one, HEAD // 2, 1) * sin
                        q[pl.ds(t * (TILE // HEAD) + i, rows, stride=8), :] = turned.astype(BF16).astype(F32)
        for i in range(heads, 8):
            q[pl.ds(i, rows, stride=8), :] = jnp.zeros((rows, HEAD), F32)

        step_keys = 512

        def scores(p, dst):
            slot = lax.rem(p, PAIRS)
            first = q[pl.ds(pl.multiple_of(16 * p, 16), 8), :]
            second = q[pl.ds(pl.multiple_of(16 * p + 8, 8), 8), :]
            zero = jnp.zeros_like(first)
            both = jnp.concatenate([jnp.concatenate([first, zero], 1), jnp.concatenate([zero, second], 1)], 0).astype(BF16)
            for c in range(0, cache, step_keys):
                at = slice(c, c + step_keys)
                k2 = jnp.concatenate([keys[slot, 0, at], keys[slot, 1, at]], 1)
                dst[:, at] = lax.dot_general(both, k2, (((1,), (1,)), ((), ())), preferred_element_type=F32)

        def weighted(p, src):
            slot = lax.rem(p, PAIRS)
            s = src[...]
            e = jnp.exp((s - jnp.max(s, -1, keepdims=True)) * HEAD**-0.5)
            weights = (e * (1 / jnp.sum(e, -1, keepdims=True))).astype(BF16)
            v2 = jnp.concatenate([values[slot, 0], values[slot, 1]], 1)
            o = dot(weights, v2)
            q[pl.ds(pl.multiple_of(16 * p, 16), 8), :] = o[:8, :HEAD]
            q[pl.ds(pl.multiple_of(16 * p + 8, 8), 8), :] = o[8:, HEAD:]

        with scope("k0_wait"):
            k_copy(0).wait()
        with scope("scores0"):
            scores(0, score_a)
        k_copy(PAIRS).start()
        with scope("barrier"):
            pl.semaphore_wait(pltpu.get_barrier_semaphore(), chips)

        def trip(i, last):
            p = 2 * i
            with scope("trip_wait"):
                k_copy(p + 1).wait()
                if not last:
                    k_copy(p + 2).wait()
                v_copy(p).wait()
                v_copy(p + 1).wait()
            with scope("trip"):
                weighted(p, score_a)
                scores(p + 1, score_b)
                if not last:
                    scores(p + 2, score_a)
                weighted(p + 1, score_b)

        @pl.loop(0, trips - 1)
        def _(i):
            trip(i, False)
            for s in range(2):
                pl.when(2 * i + s + PAIRS < pairs)(lambda s=s: v_copy(2 * i + s + PAIRS).start())
                pl.when(2 * i + s + 1 + PAIRS < pairs)(lambda s=s: k_copy(2 * i + s + 1 + PAIRS).start())

            pl.when((i >= early_trip - WO_AHEAD) & (i < early_trip - WO_AHEAD + chunks))(lambda: wo_start(i - (early_trip - WO_AHEAD)))
            pl.when(i >= trips - free_first)(lambda: mlp_start(i - (trips - free_first)))

            pl.when(i == early_trip)(lambda: gather_heads(0, early))
            sums[0].stages(i, early_lags)

        mlp_start(free_first - 1)
        trip(trips - 1, True)
        gather_heads(early, late)

    def rest(down):
        def d_copy(c):
            slot = lax.rem(c, DSLOTS)
            return pltpu.make_async_copy(wd_hbm.at[:, pl.ds(pl.multiple_of(c * chunk, chunk), chunk)], down.at[slot], d_sem.at[slot])

        for c in range(DSLOTS):
            d_copy(c).start()

        first, second = sums
        even = chunks // 2 * 2

        @pl.loop(0, even, step=2)
        def _(c):
            second.stage_a(c, c + 1)

            @pl.when(c >= 2)
            def _():
                second.stage_b(c - 2)
                second.stage_b(c - 1)

        pl.loop(even, chunks)(second.stage_a)

        @pl.loop(free_first, GSLOTS // 2)
        def _(j):
            mlp_start(j)

        pl.loop(even - 2, even)(second.stage_b)
        pl.loop(early_done[2], chunks)(first.stage_c)
        pl.loop(even, chunks)(second.stage_b)
        pl.loop(0, chunks)(second.stage_c)
        pl.loop(early_done[3], chunks)(first.stage_d)
        pl.loop(0, chunks)(second.stage_d)

        for one in sums:
            pl.loop(0, chunks)(one.finish)
            one.drain()

        with scope("norm_m"):
            normed(h, 1)

        @pl.loop(0, mlp_tiles // 2, step=MLP_STEP)
        def _(j):
            with scope("mlp_wait"):
                for s in range(MLP_STEP):
                    mlp_copy(wg_hbm, 2 * (j + s)).wait()
                    mlp_copy(wu_hbm, 2 * (j + s) + 1).wait()
            with scope("mlp"):
                for s in range(MLP_STEP):
                    gate = dot(act[...], slots[mlp_slot(2 * (j + s))])
                    up = dot(act[...], slots[mlp_slot(2 * (j + s) + 1)])
                    hidden[:, pl.ds(pl.multiple_of((j + s) * TILE, TILE), TILE)] = (gate * (1 / (1 + jnp.exp(-gate))) * up).astype(BF16)

            for s in range(MLP_STEP):
                pl.when(2 * (j + s) + GSLOTS < mlp_tiles)(lambda s=s: mlp_start(j + s + GSLOTS // 2))

        def down_term(c):
            with scope("down_wait"):
                d_copy(c).wait()
            slot = lax.rem(c, DSLOTS)
            term = jnp.concatenate([dot(hidden[...], down[slot, :, at : at + 256]) for at in range(0, chunk, 256)], 1)

            @pl.when(c + DSLOTS < chunks)
            def _():
                d_copy(c + DSLOTS).start()

            return term

        y = Summed("y", 0, 0, rows, down_term, h, states)

        @pl.loop(0, chunks + Y_LAGS[-1])
        def _(i):
            y.stages(i, Y_LAGS)

        @pl.loop(0, chunks)
        def _(c):
            y.finish(c)

        with scope("y_drain"):
            y.drain()

    pl.run_scoped(attention, pltpu.VMEM((PAIRS, 2, cache, HEAD), BF16), pltpu.VMEM((PAIRS, 2, cache, HEAD), BF16))
    pl.run_scoped(rest, pltpu.VMEM((DSLOTS, ff, chunk), BF16))


def solution(mesh):
    n = mesh.shape["tp"]

    def step(x, k_cache, v_cache, gain_a, wq, wo, gain_m, w_gate, w_up, w_down):
        rows, d = x.shape
        batch, cache, kv_heads, head = k_cache.shape
        ff = w_gate.shape[1]
        chips = n // CORES
        chunk = n * LANES
        chunks = d // chunk
        half = head // 2
        angle = (cache - 1) * THETA ** (-np.arange(half) / half)
        cos, sin = (jnp.asarray(f(angle)[None], F32) for f in (np.cos, np.sin))
        dma, vmem = pltpu.SemaphoreType.DMA, pltpu.VMEM
        in_hbm = pl.BlockSpec(memory_space=pl.ANY)
        return pl.pallas_call(
            lambda *refs: layer_kernel(n, *refs),
            out_shape=pltpu.VMEM((rows, d), x.dtype),
            in_specs=[in_hbm] * 12,
            out_specs=pl.BlockSpec(memory_space=pltpu.VMEM),
            scratch_shapes=[
                vmem((rows, d), BF16),
                vmem((rows, d), BF16),
                vmem((GSLOTS, d, TILE), BF16),
                vmem((batch * 8, head), F32),
                vmem((16, cache), F32),
                vmem((16, cache), F32),
                vmem((rows, ff), BF16),
                vmem((chunks, rows, chunk // CORES), F32),
                vmem((chunks, rows, chunk // CORES), BF16),
                vmem((chunks, rows, chunk // CORES), BF16),
                vmem((chunks, chips - 1, rows, LANES), BF16),
                vmem((chunks, chips - 1, rows, LANES), BF16),
                vmem((2, d // LANES, LANES), BF16),
                vmem((2, 1, half), F32),
                dma,
                dma((4,)),
                dma((GSLOTS,)),
                dma((chunks,)),
                dma((PAIRS,)),
                dma((PAIRS,)),
                dma((DSLOTS,)),
                dma((2, chunks)),
                dma((2, chunks)),
                dma((2, chunks)),
                dma((2, chunks)),
                dma((2, 4)),
            ],
            compiler_params=pltpu.CompilerParams(collective_id=0, has_side_effects=True, vmem_limit_bytes=65_900_000),
            name="decoder_layer",
        )(x, k_cache.reshape(batch, cache, head), v_cache.reshape(batch, cache, head), gain_a.reshape(-1, LANES), gain_m.reshape(-1, LANES), cos, sin, wq, wo, w_gate, w_up, w_down)

    states, cache, columns, rows_of = P("dp", None), P("dp", None, "tp", None), P(None, "tp"), P("tp", None)
    return jax.shard_map(
        step,
        mesh=mesh,
        in_specs=(states, cache, cache, P(None), columns, rows_of, P(None), columns, columns, rows_of),
        out_specs=states,
        check_vma=False,
    )
```
